128 devices in a mesh: rows: 16 (over z_lo, y, core), width: 8 (over z_hi, x).
Axes of the slice: x: 4, y: 4, z: 4 (z_hi: 2, z_lo: 2; z = z_hi * 2 + z_lo), core: 2. Of those that a mesh axis runs over, the one named last changes fastest.
Arguments:
- one_query: float32 [7168, 7168], P('rows', 'width'), may hold values from -0.09375 to 0.09375
- other_query: float32 [7168, 7168], P('rows', 'width'), may hold values from -0.0625 to 0.0625
- one_key: float32 [7168, 1024], P('rows', 'width'), may hold values from -0.09375 to 0.09375
- other_key: float32 [7168, 1024], P('rows', 'width'), may hold values from -0.0625 to 0.0625
- one_value: float32 [7168, 1024], P('rows', 'width'), may hold values from -0.09375 to 0.09375
- other_value: float32 [7168, 1024], P('rows', 'width'), may hold values from -0.0625 to 0.0625
- mix_share: float32 [7168], P('rows'), may hold values from 0.2 to 0.8
- norm_train: float32 [7168], P(('rows', 'width')), may hold values from 0.25 to 1.75
- norm_step: float32 [7168], P(('rows', 'width')), may hold values from -0.3 to 0.3
Outputs:
- final_query: bfloat16 [7168, 7168], P(None, 'width')
- final_key: bfloat16 [7168, 1024], P(None, 'width')
- final_value: bfloat16 [7168, 1024], P(None, 'width')
- column_query: float32 [7168], P('width')
- column_key: float32 [1024], P('width')
- column_value: float32 [1024], P('width')
- serve_norm: bfloat16 [7168], replicated
The draws below stay inside these ranges and needn't reach their ends.
All inputs are finite; a program needn't handle non-finite values.
Results may differ from the reference program's by a relative error of at most 0.001.
Values may be sent and summed in bfloat16 or wider, within the bound.
A program may use at most 128 MiB of HBM per device.

```python
import jax
import jax.numpy as jnp
from jax import lax

D_MODEL = 7168
Q_DIM = 7168
KV_DIM = 1024


def spiked(result, rng, source, target, shards_of, factor):
    owner, partner = [(jnp.arange(result.shape[position]) // (result.shape[position] // shards_of)).reshape([-1 if axis == position else 1 for axis in range(result.ndim)]) for position in (source, target)]
    chosen = jax.random.permutation(rng, shards_of)[partner]
    strong = (owner == chosen) | (owner == (partner + shards_of // 2) % shards_of)
    return jnp.where(strong, factor * result, result)


def block_levels(stream_key, shape, shards, smallest, top_value):
    def one(position, shards_of):
        heights = jax.random.uniform(jax.random.fold_in(jax.random.fold_in(stream_key, 6), position), (shards_of,), jnp.float32, smallest / len(shards), top_value / len(shards))
        return jnp.repeat(jnp.exp(heights), shape[position] // shards_of).reshape((-1,) + (1,) * (len(shape) - position - 1))

    loudness = one(*shards[0])
    for cut in shards[1:]:
        loudness = loudness * one(*cut)
    return loudness


def bell_draw(rng, dims, deviation, most, cuts=(), dtype=jnp.bfloat16):
    entries = jax.random.normal(rng, dims, jnp.float32) * deviation
    if len(cuts) > 0:
        entries = block_levels(rng, dims, cuts, -0.22, 0.18) * entries
    return jnp.clip(entries, min=-most, max=most).astype(dtype)


def heavy_noise(key, extent, scale, most, split, heavy, dtype=jnp.bfloat16):
    values = scale * jax.random.normal(key, extent, jnp.float32)
    if split:
        values = values * block_levels(key, extent, split, -0.22, 0.18)
    return jnp.clip(spiked(values, jax.random.fold_in(key, 3), *heavy), -most, most).astype(dtype)


def setup_inputs(seed: int = 0) -> dict:
    seeds = jax.random.split(jax.random.key(seed), 10)
    return {
        "one_query": heavy_noise(seeds[0], (D_MODEL, Q_DIM), D_MODEL ** -0.5, 0.09375, ((0, 16), (1, 8)), (0, 1, 16, 2.0), jnp.float32),
        "other_query": bell_draw(seeds[1], (D_MODEL, Q_DIM), D_MODEL ** -0.5, 0.0625, ((0, 16), (1, 8)), jnp.float32),
        "one_key": heavy_noise(seeds[2], (D_MODEL, KV_DIM), D_MODEL ** -0.5, 0.09375, ((0, 16), (1, 8)), (0, 1, 16, 2.0), jnp.float32),
        "other_key": bell_draw(seeds[3], (D_MODEL, KV_DIM), D_MODEL ** -0.5, 0.0625, ((0, 16), (1, 8)), jnp.float32),
        "one_value": heavy_noise(seeds[4], (D_MODEL, KV_DIM), D_MODEL ** -0.5, 0.09375, ((0, 16), (1, 8)), (0, 1, 16, 2.0), jnp.float32),
        "other_value": bell_draw(seeds[5], (D_MODEL, KV_DIM), D_MODEL ** -0.5, 0.0625, ((0, 16), (1, 8)), jnp.float32),
        "mix_share": jnp.clip(0.2 + 0.6 * jax.random.uniform(seeds[6], (D_MODEL,), jnp.float32) ** block_levels(seeds[6], (D_MODEL,), ((0, 16),), -0.2, 0.2), 0.2, 0.8),
        "norm_train": jnp.clip(1.0 + 0.15 * jax.random.normal(seeds[7], (D_MODEL,), jnp.float32), 0.25, 1.75),
        "norm_step": jnp.clip(jax.random.uniform(seeds[8], (D_MODEL,), jnp.float32, -0.3, 0.3) * block_levels(seeds[8], (D_MODEL,), ((0, 128),), -0.4, 0.0), -0.3, 0.3),
    }


def reference(one_query, other_query, one_key, other_key, one_value, other_value, mix_share, norm_train, norm_step):
    result_query = mix_share[:, None] * one_query + (1.0 - mix_share[:, None]) * other_query
    result_key = mix_share[:, None] * one_key + (1.0 - mix_share[:, None]) * other_key
    result_value = mix_share[:, None] * one_value + (1.0 - mix_share[:, None]) * other_value
    column_query = jnp.sqrt(lax.optimization_barrier(jnp.sum(result_query * result_query, axis=0)))
    final_query = (result_query / column_query).astype(jnp.bfloat16)
    column_key = jnp.sqrt(lax.optimization_barrier(jnp.sum(result_key * result_key, axis=0)))
    final_key = (result_key / column_key).astype(jnp.bfloat16)
    column_value = jnp.sqrt(lax.optimization_barrier(jnp.sum(result_value * result_value, axis=0)))
    final_value = (result_value / column_value).astype(jnp.bfloat16)
    serve_norm = (norm_train + norm_step).astype(jnp.bfloat16)
    return (final_query, final_key, final_value, column_query, column_key, column_value, serve_norm)
```

```python
import functools

import jax
import jax.numpy as jnp
from jax import lax
from jax.experimental import pallas as pl
from jax.experimental.pallas import tpu as pltpu
from jax.sharding import PartitionSpec as P

MESH = pl.DeviceIdType.MESH
HBM = pltpu.MemorySpace.HBM
VMEM = pltpu.MemorySpace.VMEM

UNITS = (5, 4, 5, 5, 4, 5)
OFFSETS = (0, 5, 9, 14, 19, 23)
UNIT = 16
BLOCK = 448
PIECE = 112

UP = (
    [(0, 0, c) for c in (0, 1, 2, 3, 4, 5)]
    + [(-1, 0, c) for c in (0, 1, 2)]
    + [(0, 1, c) for c in (3, 4)]
    + [(-1, 1, c) for c in (0, 1, 2)]
)
DOWN = (
    [(0, 0, c) for c in (3, 4, 5, 0, 1, 2)]
    + [(1, 0, c) for c in (3, 4, 5)]
    + [(0, 1, c) for c in (0, 1)]
    + [(1, 1, c) for c in (3, 4, 5)]
)
ACROSS = (
    [(0, 0, c) for c in (0, 3, 1, 4, 2, 5)]
    + [(-1, 0, 0), (1, 0, 3), (-1, 0, 1), (1, 0, 4), (-1, 0, 2), (1, 0, 5), (-1, 0, 5), (1, 0, 2)]
)
SENT = (UP, DOWN, ACROSS)
SHIFT = ((1, 0), (-1, 0), (0, 1))
STEPS = len(UP)
AHEAD = 3


def arriving(link, step):
    dy, dz, chunk = SENT[link][step]
    sy, sz = SHIFT[link]
    return ((dy - sy) % 4, (dz - sz) % 2, chunk)


ARRIVAL = {arriving(l, s): (l, s) for l in range(3) for s in range(STEPS)}
EVENTS = [(0, 0, c) for c in range(6)]


def gather_kernel(
    one_query,
    other_query,
    one_key,
    other_key,
    one_value,
    other_value,
    share,
    train,
    step_gain,
    gathered,
    scales,
    gain,
    first,
    second,
    share_row,
    share_tile,
    sums,
    inverse,
    gain_tile,
    gain_rows,
    gain_flat,
    load_sem,
    sum_send,
    sum_recv,
    across_send,
    across_recv,
    gain_send,
    gain_recv,
    link_send,
    link_recv,
    core_send,
    core_recv,
):
    me = lax.axis_index("rows")
    column = lax.axis_index("width")
    core = lax.rem(me, 2)
    y = lax.rem(me // 2, 4)
    z = me // 8

    def device(dy, dz, on):
        return lax.rem(z + dz + 2, 2) * 8 + lax.rem(y + dy + 4, 4) * 2 + on

    pieces = BLOCK // PIECE
    sources = (
        (one_query, first, 0, 896),
        (other_query, second, 0, 896),
        (one_key, first, 896, 128),
        (other_key, second, 896, 128),
        (one_value, first, 1024, 128),
        (other_value, second, 1024, 128),
    )

    def load(piece, number):
        source, target, at, width = sources[number]
        rows = pl.ds(piece * PIECE, PIECE)
        return pltpu.make_async_copy(
            source.at[rows, :], target.at[rows, pl.ds(at, width)], load_sem.at[piece, number]
        )

    for piece in range(pieces):
        for number in range(6):
            load(piece, number).start()

    barrier = pltpu.get_barrier_semaphore()
    for k in range(1, 16):
        pl.semaphore_signal(barrier, inc=1, device_id=(lax.rem(me + k, 16), column), device_id_type=MESH)
    for k in range(1, 8):
        pl.semaphore_signal(barrier, inc=1, device_id=(me, lax.rem(column + k, 8)), device_id_type=MESH)

    share_row[...] = jnp.zeros_like(share_row)
    share_row[:, 0:BLOCK] = share[...]
    for part in range(4):
        lanes = share_row[:, part * 128 : (part + 1) * 128]
        share_tile[pl.ds(part * 128, 128), :] = jnp.transpose(jnp.broadcast_to(lanes, (128, 128)))

    gain_tile[...] = jnp.zeros_like(gain_tile)
    gain_tile[0:1, 0:56] = (train[...] + step_gain[...]).astype(jnp.bfloat16).astype(jnp.float32)
    place = lax.rem(56 * (lax.rem(me, 2) * 8 + column), 128)
    gain_rows[me, column] = pltpu.roll(gain_tile[...], place, 1)[0:1, :]

    def mix(piece):
        def body(i, total):
            total = list(total)
            for half in range(2):
                rows = pl.ds(pl.multiple_of(piece * PIECE + i * 16 + half * 8, 8), 8)
                mine = share_tile[rows, :]
                rest = 1.0 - mine
                for j in range(9):
                    lanes = slice(j * 128, (j + 1) * 128)
                    result = mine * first[rows, lanes] + rest * second[rows, lanes]
                    first[rows, lanes] = result
                    total[j] = total[j] + result * result
            return tuple(total)

        return body

    total = tuple(jnp.zeros((8, 128), jnp.float32) for _ in range(9))
    for piece in range(pieces):
        for number in range(6):
            load(piece, number).wait()
        total = lax.fori_loop(0, PIECE // 16, mix(piece), total)
    for j in range(9):
        sums[me, j] = jnp.sum(total[j], axis=0, keepdims=True)

    pl.semaphore_wait(barrier, 22)

    def send_sum(k, owner):
        return pltpu.make_async_remote_copy(
            src_ref=sums.at[owner],
            dst_ref=sums.at[owner],
            send_sem=sum_send.at[k],
            recv_sem=sum_recv.at[k],
            device_id=(lax.rem(me + k, 16), column),
            device_id_type=MESH,
        )

    def send_across(k, owner):
        return pltpu.make_async_remote_copy(
            src_ref=gain_rows.at[me, owner],
            dst_ref=gain_rows.at[me, owner],
            send_sem=across_send.at[k],
            recv_sem=across_recv.at[k],
            device_id=(me, lax.rem(column + k, 8)),
            device_id_type=MESH,
        )

    def send_gain(k, owner):
        return pltpu.make_async_remote_copy(
            src_ref=gain_rows.at[owner],
            dst_ref=gain_rows.at[owner],
            send_sem=gain_send.at[k],
            recv_sem=gain_recv.at[k],
            device_id=(lax.rem(me + k, 16), column),
            device_id_type=MESH,
        )

    for k in range(1, 16):
        send_sum(k, me).start()
    for k in range(1, 8):
        send_across(k, column).start()
    for k in range(1, 16):
        send_sum(k, lax.rem(me + 16 - k, 16)).wait_recv()

    grand = [sums[0, j] for j in range(9)]
    for other in range(1, 16):
        grand = [grand[j] + sums[other, j] for j in range(9)]
    for j in range(9):
        scale = jnp.sqrt(grand[j])
        scales[j] = scale
        inverse[j] = 1.0 / scale

    def rows_of(dy, dz, chunk, on):
        start = device(dy, dz, on) * BLOCK + OFFSETS[chunk] * UNIT
        return pl.ds(pl.multiple_of(start, UNIT), UNITS[chunk] * UNIT)

    def link_copy(link, step, item):
        rows = rows_of(*item, core)
        sy, sz = SHIFT[link]
        return pltpu.make_async_remote_copy(
            src_ref=gathered.at[rows, :],
            dst_ref=gathered.at[rows, :],
            send_sem=link_send.at[link, step],
            recv_sem=link_recv.at[link, step],
            device_id=(device(sy, sz, core), column),
            device_id_type=MESH,
        )

    events = []

    def core_copy(event, item, on):
        rows = rows_of(*item, on)
        return pltpu.make_async_remote_copy(
            src_ref=gathered.at[rows, :],
            dst_ref=gathered.at[rows, :],
            send_sem=core_send.at[event],
            recv_sem=core_recv.at[event],
            device_id=(device(0, 0, 1 - core), column),
            device_id_type=MESH,
        )

    def hand_over(item):
        core_copy(len(events), item, core).start()
        events.append(item)

    def normalise(chunk):
        def body(i, _):
            at = pl.multiple_of(OFFSETS[chunk] * UNIT + i * UNIT, UNIT)
            to = pl.multiple_of(me * BLOCK + OFFSETS[chunk] * UNIT + i * UNIT, UNIT)
            for j in range(9):
                lanes = slice(j * 128, (j + 1) * 128)
                gathered[pl.ds(to, UNIT), lanes] = (first[pl.ds(at, UNIT), lanes] * inverse[j]).astype(jnp.bfloat16)
            return 0

        lax.fori_loop(0, UNITS[chunk], body, 0)

    for chunk in (0, 3, 1, 4, 2, 5):
        normalise(chunk)

    arrived = set()

    def receive(link, step):
        if (link, step) in arrived:
            return
        arrived.add((link, step))
        item = arriving(link, step)
        link_copy(link, step, item).wait_recv()
        hand_over(item)

    for step in range(STEPS):
        for link in range(3):
            if step >= AHEAD:
                link_copy(link, step - AHEAD, SENT[link][step - AHEAD]).wait_send()
            dy, dz, chunk = SENT[link][step]
            if (dy, dz) != (0, 0):
                receive(*ARRIVAL[dy % 4, dz % 2, chunk])
            link_copy(link, step, SENT[link][step]).start()
        if step < 6:
            hand_over((0, 0, step))
        if step == 2:
            for k in range(1, 8):
                send_across(k, lax.rem(column + 8 - k, 8)).wait_recv()
            for k in range(1, 16):
                send_gain(k, me).start()
        if step >= AHEAD:
            for link in range(3):
                receive(link, step - AHEAD)

    for k in range(1, 16):
        send_gain(k, lax.rem(me + 16 - k, 16)).wait_recv()
    lane = lax.broadcasted_iota(jnp.int32, (1, 128), 1)
    for group in range(8):
        rows = [jnp.zeros((1, 128), jnp.float32) for _ in range(8)]
        for j in range(16):
            values = gain_rows[group * 2 + j // 8, j % 8]
            row, at = (56 * j) // 128, (56 * j) % 128
            rows[row] = jnp.where((lane >= at) & (lane < at + 56), values, rows[row])
            if at + 56 > 128:
                rows[row + 1] = jnp.where(lane < at + 56 - 128, values, rows[row + 1])
        for row in range(7):
            gain_flat[group * 7 + row : group * 7 + row + 1, :] = rows[row]
    gain[...] = gain_flat[...].astype(jnp.bfloat16)

    for step in range(STEPS - AHEAD, STEPS):
        for link in range(3):
            receive(link, step)
    for event, item in enumerate(events):
        core_copy(event, item, 1 - core).wait_recv()
    for step in range(STEPS - AHEAD, STEPS):
        for link in range(3):
            link_copy(link, step, SENT[link][step]).wait_send()
    for event, item in enumerate(events):
        core_copy(event, item, core).wait_send()
    for k in range(1, 16):
        send_sum(k, me).wait_send()
        send_gain(k, me).wait_send()
    for k in range(1, 8):
        send_across(k, column).wait_send()


def write_kernel(gathered, query, key, value, sem):
    copies = []
    parts = 8
    rows = gathered.shape[0] // parts
    for part in range(parts):
        for target, at, width in ((query, 0, 896), (key, 896, 128), (value, 1024, 128)):
            copies.append(
                pltpu.make_async_copy(
                    gathered.at[pl.ds(part * rows, rows), pl.ds(at, width)],
                    target.at[pl.ds(part * rows, rows), :],
                    sem.at[len(copies)],
                )
            )
    for copy in copies:
        copy.start()
    for copy in copies:
        copy.wait()


def shards(
    one_query,
    other_query,
    one_key,
    other_key,
    one_value,
    other_value,
    mix_share,
    norm_train,
    norm_step,
):
    dma = pltpu.SemaphoreType.DMA
    weights = [
        pltpu.with_memory_space_constraint(w, HBM)
        for w in (one_query, other_query, one_key, other_key, one_value, other_value)
    ]
    gathered, scales, gain = pl.pallas_call(
        gather_kernel,
        out_shape=(
            jax.ShapeDtypeStruct((7168, 1152), jnp.bfloat16),
            jax.ShapeDtypeStruct((9, 1, 128), jnp.float32),
            jax.ShapeDtypeStruct((56, 128), jnp.bfloat16),
        ),
        in_specs=[pl.BlockSpec(memory_space=HBM)] * 6 + [pl.BlockSpec(memory_space=VMEM)] * 3,
        out_specs=(pl.BlockSpec(memory_space=VMEM),) * 3,
        scratch_shapes=[
            pltpu.VMEM((448, 1152), jnp.float32),
            pltpu.VMEM((448, 1152), jnp.float32),
            pltpu.VMEM((1, 512), jnp.float32),
            pltpu.VMEM((512, 128), jnp.float32),
            pltpu.VMEM((16, 9, 1, 128), jnp.float32),
            pltpu.VMEM((9, 1, 128), jnp.float32),
            pltpu.VMEM((8, 128), jnp.float32),
            pltpu.VMEM((16, 8, 1, 128), jnp.float32),
            pltpu.VMEM((56, 128), jnp.float32),
            dma((4, 6)),
            dma((16,)),
            dma((16,)),
            dma((8,)),
            dma((8,)),
            dma((16,)),
            dma((16,)),
            dma((3, STEPS)),
            dma((3, STEPS)),
            dma((48,)),
            dma((48,)),
        ],
        compiler_params=pltpu.CompilerParams(
            collective_id=0, has_side_effects=True, vmem_limit_bytes=32 << 20
        ),
    )(
        *weights,
        mix_share.reshape(1, 448),
        norm_train.reshape(1, 56),
        norm_step.reshape(1, 56),
    )
    query, key, value = pl.pallas_call(
        write_kernel,
        out_shape=(
            jax.ShapeDtypeStruct((7168, 896), jnp.bfloat16),
            jax.ShapeDtypeStruct((7168, 128), jnp.bfloat16),
            jax.ShapeDtypeStruct((7168, 128), jnp.bfloat16),
        ),
        in_specs=[pl.BlockSpec(memory_space=VMEM)],
        out_specs=(pl.BlockSpec(memory_space=HBM),) * 3,
        scratch_shapes=[dma((24,))],
        compiler_params=pltpu.CompilerParams(vmem_limit_bytes=20 << 20),
    )(gathered)
    flat = scales.reshape(1152)
    return (query, key, value, flat[:896], flat[896:1024], flat[1024:], gain.reshape(7168))


def solution(mesh):
    in_specs = (
        P("rows", "width"),
        P("rows", "width"),
        P("rows", "width"),
        P("rows", "width"),
        P("rows", "width"),
        P("rows", "width"),
        P("rows"),
        P(("rows", "width")),
        P(("rows", "width")),
    )
    out_specs = (
        P(None, "width"),
        P(None, "width"),
        P(None, "width"),
        P("width"),
        P("width"),
        P("width"),
        P(),
    )
    return jax.shard_map(shards, mesh=mesh, in_specs=in_specs, out_specs=out_specs, check_vma=False)
```

```python
import functools

import jax
import jax.numpy as jnp
from jax import lax
from jax.experimental import pallas as pl
from jax.experimental.pallas import tpu as pltpu
from jax.sharding import PartitionSpec as P

MESH = pl.DeviceIdType.MESH
HBM = pltpu.MemorySpace.HBM
VMEM = pltpu.MemorySpace.VMEM

UNITS = (5, 4, 5, 5, 4, 5)
OFFSETS = (0, 5, 9, 14, 19, 23)
UNIT = 16
BLOCK = 448
PIECE = 112

UP = (
    [(0, 0, c) for c in (0, 1, 2, 3, 4, 5)]
    + [(-1, 0, c) for c in (0, 1, 2)]
    + [(0, 1, c) for c in (3, 4)]
    + [(-1, 1, c) for c in (0, 1, 2)]
)
DOWN = (
    [(0, 0, c) for c in (3, 4, 5, 0, 1, 2)]
    + [(1, 0, c) for c in (3, 4, 5)]
    + [(0, 1, c) for c in (0, 1)]
    + [(1, 1, c) for c in (3, 4, 5)]
)
ACROSS = (
    [(0, 0, c) for c in (0, 3, 1, 4, 2, 5)]
    + [(-1, 0, 0), (1, 0, 3), (-1, 0, 1), (1, 0, 4), (-1, 0, 2), (1, 0, 5), (-1, 0, 5), (1, 0, 2)]
)
SENT = (UP, DOWN, ACROSS)
SHIFT = ((1, 0), (-1, 0), (0, 1))
STEPS = len(UP)
AHEAD = 3
GATE = 5
GAIN_STEPS = (4, 7, 8, 11)
FARTHEST = ((2, 1), (1, 1), (3, 1), (2, 0), (1, 0), (3, 0), (0, 1), (0, 0))


def arriving(link, step):
    dy, dz, chunk = SENT[link][step]
    sy, sz = SHIFT[link]
    return ((dy - sy) % 4, (dz - sz) % 2, chunk)


ARRIVAL = {arriving(l, s): (l, s) for l in range(3) for s in range(STEPS)}
EVENTS = [(0, 0, c) for c in range(6)]


def gather_kernel(
    one_query,
    other_query,
    one_key,
    other_key,
    one_value,
    other_value,
    share_input,
    train_input,
    step_input,
    gathered,
    scale_query,
    scale_key,
    scale_value,
    gain,
    first,
    second,
    share,
    train,
    step_gain,
    share_row,
    share_tile,
    sums,
    inverse,
    gain_tile,
    gain_rows,
    gain_flat,
    load_sem,
    small_sem,
    entered,
    sum_send,
    sum_recv,
    row_send,
    row_recv,
    gate_send,
    gate_recv,
    gain_send,
    gain_recv,
    link_send,
    link_recv,
    core_send,
    core_recv,
):
    me = lax.axis_index("rows")
    column = lax.axis_index("width")
    core = lax.rem(me, 2)
    y = lax.rem(me // 2, 4)
    z = me // 8

    def device(dy, dz, on):
        return lax.rem(z + dz + 2, 2) * 8 + lax.rem(y + dy + 4, 4) * 2 + on

    pieces = BLOCK // PIECE
    sources = (
        (one_query, first, 0, 896),
        (other_query, second, 0, 896),
        (one_key, first, 896, 128),
        (other_key, second, 896, 128),
        (one_value, first, 1024, 128),
        (other_value, second, 1024, 128),
    )

    def load(piece, number):
        source, target, at, width = sources[number]
        rows = pl.ds(piece * PIECE, PIECE)
        return pltpu.make_async_copy(
            source.at[rows, :], target.at[rows, pl.ds(at, width)], load_sem.at[piece, number]
        )

    small = [
        pltpu.make_async_copy(source, target, small_sem.at[number])
        for number, (source, target) in enumerate(
            ((share_input, share), (train_input, train), (step_input, step_gain))
        )
    ]
    for copy in small:
        copy.start()
    for piece in range(pieces):
        for number in range(6):
            load(piece, number).start()

    at_gate = me == GATE
    barrier = pltpu.get_barrier_semaphore()
    for k in range(1, 16):
        peer = lax.rem(me + k, 16)

        @pl.when(peer != GATE)
        def _():
            pl.semaphore_signal(barrier, inc=1, device_id=(peer, column), device_id_type=MESH)

    @pl.when(at_gate)
    def _():
        for k in range(1, 8):
            pl.semaphore_signal(barrier, inc=1, device_id=(me, lax.rem(column + k, 8)), device_id_type=MESH)

    for copy in small:
        copy.wait()

    share_row[...] = jnp.zeros_like(share_row)
    share_row[:, 0:BLOCK] = share[...]
    for part in range(4):
        lanes = share_row[:, part * 128 : (part + 1) * 128]
        share_tile[pl.ds(part * 128, 128), :] = jnp.transpose(jnp.broadcast_to(lanes, (128, 128)))

    gain_tile[...] = jnp.zeros_like(gain_tile)
    gain_tile[0:1, 0:56] = (train[...] + step_gain[...]).astype(jnp.bfloat16).astype(jnp.float32)
    place = lax.rem(56 * (lax.rem(me, 2) * 8 + column), 128)
    gain_rows[column, me] = pltpu.roll(gain_tile[...], place, 1)[0:1, :]

    def mix(piece):
        def body(i, total):
            total = list(total)
            for half in range(2):
                rows = pl.ds(pl.multiple_of(piece * PIECE + i * 16 + half * 8, 8), 8)
                mine = share_tile[rows, :]
                rest = 1.0 - mine
                for j in range(9):
                    lanes = slice(j * 128, (j + 1) * 128)
                    result = mine * first[rows, lanes] + rest * second[rows, lanes]
                    first[rows, lanes] = result
                    total[j] = total[j] + result * result
            return tuple(total)

        return body

    total = tuple(jnp.zeros((8, 128), jnp.float32) for _ in range(9))
    for piece in range(pieces):
        for number in range(6):
            load(piece, number).wait()
        total = lax.fori_loop(0, PIECE // 16, mix(piece), total)
    for j in range(9):
        sums[me, j] = jnp.sum(total[j], axis=0, keepdims=True)

    @pl.when(jnp.logical_not(at_gate))
    def _():
        pl.semaphore_wait(barrier, 15)

    @pl.when(me == GATE - 1)
    def _():
        pl.semaphore_signal(entered, inc=1, device_id=(GATE, column), device_id_type=MESH)

    @pl.when(at_gate)
    def _():
        pl.semaphore_wait(entered, 1)

    others = [(dy, dz, on) for dy, dz in FARTHEST for on in (0, 1) if (dy, dz, on) != (0, 0, 0)]

    def send_sum(k, owner):
        dy, dz, on = others[k]
        return pltpu.make_async_remote_copy(
            src_ref=sums.at[owner],
            dst_ref=sums.at[owner],
            send_sem=sum_send.at[k],
            recv_sem=sum_recv.at[k],
            device_id=(device(dy, dz, lax.rem(core + on, 2)), column),
            device_id_type=MESH,
        )

    for k in range(15):
        send_sum(k, me).start()

    def send_row(owner):
        return pltpu.make_async_remote_copy(
            src_ref=gain_rows.at[column, owner],
            dst_ref=gain_rows.at[column, owner],
            send_sem=row_send,
            recv_sem=row_recv.at[owner],
            device_id=(GATE, column),
            device_id_type=MESH,
        )

    def send_group(k, owner):
        return pltpu.make_async_remote_copy(
            src_ref=gain_rows.at[owner],
            dst_ref=gain_rows.at[owner],
            send_sem=gate_send.at[k],
            recv_sem=gate_recv.at[k],
            device_id=(GATE, lax.rem(column + k, 8)),
            device_id_type=MESH,
        )

    def send_gain(k, to):
        return pltpu.make_async_remote_copy(
            src_ref=gain,
            dst_ref=gain,
            send_sem=gain_send.at[k],
            recv_sem=gain_recv,
            device_id=(to, column),
            device_id_type=MESH,
        )

    @pl.when(jnp.logical_not(at_gate))
    def _():
        send_row(me).start()

    for k in range(15):
        dy, dz, on = others[k]
        send_sum(k, device(-dy, -dz, lax.rem(core + on, 2))).wait_recv()

    grand = [sums[0, j] for j in range(9)]
    for other in range(1, 16):
        grand = [grand[j] + sums[other, j] for j in range(9)]
    for j in range(9):
        scale = jnp.sqrt(grand[j])
        if j < 7:
            scale_query[j : j + 1, :] = scale
        elif j == 7:
            scale_key[...] = scale
        else:
            scale_value[...] = scale
        inverse[j] = 1.0 / scale

    def compose():
        lane = lax.broadcasted_iota(jnp.int32, (1, 128), 1)
        for group in range(8):
            rows = [jnp.zeros((1, 128), jnp.float32) for _ in range(8)]
            for j in range(16):
                values = gain_rows[j % 8, group * 2 + j // 8]
                row, at = (56 * j) // 128, (56 * j) % 128
                rows[row] = jnp.where((lane >= at) & (lane < at + 56), values, rows[row])
                if at + 56 > 128:
                    rows[row + 1] = jnp.where(lane < at + 56 - 128, values, rows[row + 1])
            for row in range(7):
                gain_flat[group * 7 + row : group * 7 + row + 1, :] = rows[row]
        gain[...] = gain_flat[...].astype(jnp.bfloat16)

    spread = [to for to in range(16) if to % 2 == GATE % 2 and to != GATE] + [GATE - 1]

    def rows_of(dy, dz, chunk, on):
        start = device(dy, dz, on) * BLOCK + OFFSETS[chunk] * UNIT
        return pl.ds(pl.multiple_of(start, UNIT), UNITS[chunk] * UNIT)

    def link_copy(link, step, item):
        rows = rows_of(*item, core)
        sy, sz = SHIFT[link]
        return pltpu.make_async_remote_copy(
            src_ref=gathered.at[rows, :],
            dst_ref=gathered.at[rows, :],
            send_sem=link_send.at[link, step],
            recv_sem=link_recv.at[link, step],
            device_id=(device(sy, sz, core), column),
            device_id_type=MESH,
        )

    events = []

    def core_copy(event, item, on):
        rows = rows_of(*item, on)
        return pltpu.make_async_remote_copy(
            src_ref=gathered.at[rows, :],
            dst_ref=gathered.at[rows, :],
            send_sem=core_send.at[event],
            recv_sem=core_recv.at[event],
            device_id=(device(0, 0, 1 - core), column),
            device_id_type=MESH,
        )

    def hand_over(item):
        core_copy(len(events), item, core).start()
        events.append(item)

    def normalise(chunk):
        def body(i, _):
            at = pl.multiple_of(OFFSETS[chunk] * UNIT + i * UNIT, UNIT)
            to = pl.multiple_of(me * BLOCK + OFFSETS[chunk] * UNIT + i * UNIT, UNIT)
            for j in range(9):
                lanes = slice(j * 128, (j + 1) * 128)
                gathered[pl.ds(to, UNIT), lanes] = (first[pl.ds(at, UNIT), lanes] * inverse[j]).astype(jnp.bfloat16)
            return 0

        lax.fori_loop(0, UNITS[chunk], body, 0)

    for chunk in (0, 3, 1, 4, 2, 5):
        normalise(chunk)

    arrived = set()

    def receive(link, step):
        if (link, step) in arrived:
            return
        arrived.add((link, step))
        item = arriving(link, step)
        link_copy(link, step, item).wait_recv()
        hand_over(item)

    for step in range(STEPS):
        for link in range(3):
            if step >= AHEAD:
                link_copy(link, step - AHEAD, SENT[link][step - AHEAD]).wait_send()
            dy, dz, chunk = SENT[link][step]
            if (dy, dz) != (0, 0):
                receive(*ARRIVAL[dy % 4, dz % 2, chunk])
            link_copy(link, step, SENT[link][step]).start()
        if step < 6:
            hand_over((0, 0, step))
        if step == GAIN_STEPS[0]:

            @pl.when(at_gate)
            def _():
                for owner in range(16):
                    if owner != GATE:
                        send_row(owner).wait_recv()
                pl.semaphore_wait(barrier, 7)
                for k in range(1, 8):
                    send_group(k, column).start()

        if step == GAIN_STEPS[1]:

            @pl.when(at_gate)
            def _():
                for k in range(1, 8):
                    send_group(k, lax.rem(column + 8 - k, 8)).wait_recv()
                compose()

        if step == GAIN_STEPS[2]:

            @pl.when(at_gate)
            def _():
                for k, to in enumerate(spread):
                    send_gain(k, to).start()

        if step == GAIN_STEPS[3]:

            @pl.when(jnp.logical_and(jnp.logical_not(at_gate), core == GATE % 2))
            def _():
                send_gain(0, me).wait_recv()
                send_gain(0, device(0, 0, 1 - core)).start()

        if step >= AHEAD:
            for link in range(3):
                receive(link, step - AHEAD)

    for step in range(STEPS - AHEAD, STEPS):
        for link in range(3):
            receive(link, step)
    for event, item in enumerate(events):
        core_copy(event, item, 1 - core).wait_recv()
    for step in range(STEPS - AHEAD, STEPS):
        for link in range(3):
            link_copy(link, step, SENT[link][step]).wait_send()
    for event, item in enumerate(events):
        core_copy(event, item, core).wait_send()
    for k in range(15):
        send_sum(k, me).wait_send()

    @pl.when(core != GATE % 2)
    def _():
        send_gain(0, me).wait_recv()

    @pl.when(at_gate)
    def _():
        for k in range(1, 8):
            send_group(k, column).wait_send()
        for k, to in enumerate(spread):
            send_gain(k, to).wait_send()

    @pl.when(jnp.logical_not(at_gate))
    def _():
        send_row(me).wait_send()

        @pl.when(core == GATE % 2)
        def _():
            send_gain(0, me).wait_send()


def write_kernel(gathered, *rest):
    small, (query, key, value), outs, sem = rest[:4], rest[4:7], rest[7:11], rest[11]
    copies = []

    def copy(source, target):
        copies.append(pltpu.make_async_copy(source, target, sem.at[len(copies)]))

    parts = 8
    rows = gathered.shape[0] // parts
    for part in range(parts):
        for target, at, width in ((query, 0, 896), (key, 896, 128), (value, 1024, 128)):
            copy(gathered.at[pl.ds(part * rows, rows), pl.ds(at, width)], target.at[pl.ds(part * rows, rows), :])
    for source, target in zip(small, outs):
        copy(source, target)
    for one in copies:
        one.start()
    for one in copies:
        one.wait()


def shards(
    one_query,
    other_query,
    one_key,
    other_key,
    one_value,
    other_value,
    mix_share,
    norm_train,
    norm_step,
):
    dma = pltpu.SemaphoreType.DMA
    f32, bf16 = jnp.float32, jnp.bfloat16
    inputs = [
        pltpu.with_memory_space_constraint(x, HBM)
        for x in (
            one_query,
            other_query,
            one_key,
            other_key,
            one_value,
            other_value,
            mix_share.reshape(1, 448),
            norm_train.reshape(1, 56),
            norm_step.reshape(1, 56),
        )
    ]
    small = (
        jax.ShapeDtypeStruct((7, 128), f32),
        jax.ShapeDtypeStruct((1, 128), f32),
        jax.ShapeDtypeStruct((1, 128), f32),
        jax.ShapeDtypeStruct((56, 128), bf16),
    )
    gathered, *rest = pl.pallas_call(
        gather_kernel,
        out_shape=(jax.ShapeDtypeStruct((7168, 1152), bf16), *small),
        in_specs=[pl.BlockSpec(memory_space=HBM)] * 9,
        out_specs=(pl.BlockSpec(memory_space=VMEM),) * 5,
        scratch_shapes=[
            pltpu.VMEM((448, 1152), f32),
            pltpu.VMEM((448, 1152), f32),
            pltpu.VMEM((1, 448), f32),
            pltpu.VMEM((1, 56), f32),
            pltpu.VMEM((1, 56), f32),
            pltpu.VMEM((1, 512), f32),
            pltpu.VMEM((512, 128), f32),
            pltpu.VMEM((16, 9, 1, 128), f32),
            pltpu.VMEM((9, 1, 128), f32),
            pltpu.VMEM((8, 128), f32),
            pltpu.VMEM((8, 16, 1, 128), f32),
            pltpu.VMEM((56, 128), f32),
            dma((4, 6)),
            dma((3,)),
            pltpu.SemaphoreType.REGULAR,
            dma((15,)),
            dma((15,)),
            dma,
            dma((16,)),
            dma((8,)),
            dma((8,)),
            dma((8,)),
            dma,
            dma((3, STEPS)),
            dma((3, STEPS)),
            dma((48,)),
            dma((48,)),
        ],
        compiler_params=pltpu.CompilerParams(
            collective_id=0, has_side_effects=True, vmem_limit_bytes=32 << 20
        ),
    )(*inputs)
    query, key, value, *outs = pl.pallas_call(
        write_kernel,
        out_shape=(
            jax.ShapeDtypeStruct((7168, 896), bf16),
            jax.ShapeDtypeStruct((7168, 128), bf16),
            jax.ShapeDtypeStruct((7168, 128), bf16),
            *small,
        ),
        in_specs=[pl.BlockSpec(memory_space=VMEM)] * 5,
        out_specs=(pl.BlockSpec(memory_space=HBM),) * 7,
        scratch_shapes=[dma((28,))],
        compiler_params=pltpu.CompilerParams(vmem_limit_bytes=20 << 20),
    )(gathered, *rest)
    return (query, key, value, *(x.reshape(-1) for x in outs))


def solution(mesh):
    in_specs = (
        P("rows", "width"),
        P("rows", "width"),
        P("rows", "width"),
        P("rows", "width"),
        P("rows", "width"),
        P("rows", "width"),
        P("rows"),
        P(("rows", "width")),
        P(("rows", "width")),
    )
    out_specs = (
        P(None, "width"),
        P(None, "width"),
        P(None, "width"),
        P("width"),
        P("width"),
        P("width"),
        P(),
    )
    return jax.shard_map(shards, mesh=mesh, in_specs=in_specs, out_specs=out_specs, check_vma=False)
```

```python
import functools

import jax
import jax.numpy as jnp
from jax import lax
from jax.experimental import pallas as pl
from jax.experimental.pallas import tpu as pltpu
from jax.sharding import PartitionSpec as P

MESH = pl.DeviceIdType.MESH
HBM = pltpu.MemorySpace.HBM
VMEM = pltpu.MemorySpace.VMEM

BLOCK = 448
HALF = 224
PIECE = 112
QUERY = (0, 896)
KEYVALUE = (896, 256)
ALL = (0, 1152)
LOW = ((0, 80), (80, 144), (144, 224))
HIGH = ((224, 304), (304, 368), (368, 448))


def own(*parts):
    return [(0, 0, rows, columns) for rows, columns in parts]


def relay(dy, dz, *rows):
    return [(dy, dz, r, ALL) for r in rows]


UP = (
    own(((0, 144), KEYVALUE), ((0, 80), QUERY), ((80, 144), QUERY), (LOW[2], ALL), *((r, ALL) for r in HIGH))
    + relay(-1, 0, *LOW)
    + relay(0, 1, (224, 304), (304, 376))
    + relay(-1, 1, (0, 80), (80, 144), (144, 192), (192, 224))
)
DOWN = (
    own(((224, 368), KEYVALUE), ((224, 304), QUERY), ((304, 368), QUERY), (HIGH[2], ALL), *((r, ALL) for r in LOW))
    + relay(1, 0, *HIGH)
    + relay(0, 1, (0, 80), (80, 152))
    + relay(1, 1, (224, 304), (304, 368), (368, 416), (416, 448))
)
ACROSS = (
    own(
        ((0, 144), KEYVALUE),
        ((0, 80), QUERY),
        (HIGH[0], ALL),
        ((80, 144), QUERY),
        (HIGH[1], ALL),
        (LOW[2], ALL),
        (HIGH[2], ALL),
    )
    + relay(-1, 0, LOW[0])
    + relay(1, 0, HIGH[0])
    + relay(-1, 0, LOW[1])
    + relay(1, 0, HIGH[1])
    + relay(-1, 0, LOW[2])
    + relay(1, 0, HIGH[2])
    + relay(-1, 0, (376, 448))
    + relay(1, 0, (152, 192), (192, 224))
)
SENT = (UP, DOWN, ACROSS)
SHIFT = ((1, 0), (-1, 0), (0, 1))
STEPS = len(UP)
AHEAD = 3
SLOTS = 2 * AHEAD + 2
GATE = 5
GAIN_STEPS = (5, 8, 9, 12)
FARTHEST = ((2, 1), (1, 1), (3, 1), (2, 0), (1, 0), (3, 0), (0, 1), (0, 0))


def arriving(link, step):
    dy, dz, rows, columns = SENT[link][step]
    sy, sz = SHIFT[link]
    return ((dy - sy) % 4, (dz - sz) % 2, rows, columns)


ARRIVALS = [(l, s) for s in range(STEPS) for l in range(3)]


def needed(item):
    dy, dz, rows, _ = item
    for l, s in ARRIVALS:
        ay, az, have, _ = arriving(l, s)
        if (ay, az) == (dy % 4, dz % 2) and have[0] < rows[1] and rows[0] < have[1]:
            yield l, s


def gather_kernel(
    one_query,
    other_query,
    one_key,
    other_key,
    one_value,
    other_value,
    share_input,
    train_input,
    step_input,
    gathered,
    scale_query,
    scale_key,
    scale_value,
    gain,
    first,
    second,
    share,
    gains,
    share_row,
    share_tile,
    sums_late,
    sums_early,
    inverse,
    gain_tile,
    gain_rows,
    gain_flat,
    load_sem,
    small_sem,
    entered,
    sum_send,
    sum_recv,
    row_sem,
    gate_sem,
    gain_sem,
    link_send,
    link_recv,
    core_send,
    core_recv,
):
    me = lax.axis_index("rows")
    column = lax.axis_index("width")
    core = lax.rem(me, 2)
    y = lax.rem(me // 2, 4)
    z = me // 8

    def device(dy, dz, on):
        return lax.rem(z + dz + 2, 2) * 8 + lax.rem(y + dy + 4, 4) * 2 + on

    small = [
        pltpu.make_async_copy(share_input, share, small_sem.at[0]),
        pltpu.make_async_copy(train_input, gains.at[0], small_sem.at[1]),
        pltpu.make_async_copy(step_input, gains.at[1], small_sem.at[1]),
    ]
    pieces = BLOCK // PIECE
    small[0].start()
    for source, target, at in (
        (one_key, first, 896),
        (other_key, second, 896),
        (one_value, first, 1024),
        (other_value, second, 1024),
    ):
        pltpu.make_async_copy(source, target.at[:, pl.ds(at, 128)], load_sem.at[pieces]).start()
    for piece in range(pieces):
        rows = pl.ds(piece * PIECE, PIECE)
        for source, target in ((one_query, first), (other_query, second)):
            pltpu.make_async_copy(source.at[rows, :], target.at[rows, pl.ds(0, 896)], load_sem.at[piece]).start()
    for copy in small[1:]:
        copy.start()

    def loaded(number, rows, columns):
        place = (pl.ds(0, rows), pl.ds(0, columns))
        pltpu.make_async_copy(first.at[place], second.at[place], load_sem.at[number]).wait()

    at_gate = me == GATE
    barrier = pltpu.get_barrier_semaphore()
    for k in range(1, 16):
        peer = lax.rem(me + k, 16)

        @pl.when(peer != GATE)
        def _():
            pl.semaphore_signal(barrier, inc=1, device_id=(peer, column), device_id_type=MESH)

    @pl.when(at_gate)
    def _():
        for k in range(1, 8):
            pl.semaphore_signal(barrier, inc=1, device_id=(me, lax.rem(column + k, 8)), device_id_type=MESH)

    small[0].wait()
    share_row[...] = jnp.zeros_like(share_row)
    share_row[:, 0:BLOCK] = share[...]
    for part in range(4):
        lanes = share_row[:, part * 128 : (part + 1) * 128]
        share_tile[pl.ds(part * 128, 128), :] = jnp.transpose(jnp.broadcast_to(lanes, (128, 128)))

    def mix(start, rows, tiles, total):
        def body(i, total):
            total = list(total)
            for part in range(2):
                at = pl.ds(pl.multiple_of(start + i * 16 + part * 8, 8), 8)
                mine = share_tile[at, :]
                rest = 1.0 - mine
                for n, j in enumerate(tiles):
                    lanes = slice(j * 128, (j + 1) * 128)
                    result = mine * first[at, lanes] + rest * second[at, lanes]
                    first[at, lanes] = result
                    total[n] = total[n] + result * result
            return tuple(total)

        return lax.fori_loop(0, rows // 16, body, total, unroll=2 if len(tiles) == 2 else 1)

    def zeros(n):
        return tuple(jnp.zeros((8, 128), jnp.float32) for _ in range(n))

    others = [(dy, dz, on) for dy, dz in FARTHEST for on in (0, 1) if (dy, dz, on) != (0, 0, 0)]

    def send_sum(sums, n, dy, dz, on):
        return pltpu.make_async_remote_copy(
            src_ref=sums.at[me],
            dst_ref=sums.at[me],
            send_sem=sum_send.at[n],
            recv_sem=sum_recv.at[n],
            device_id=(device(dy, dz, lax.rem(core + on, 2)), column),
            device_id_type=MESH,
        )

    def all_sums(sums, n):
        return pltpu.make_async_remote_copy(
            src_ref=sums.at[pl.ds(0, 15)],
            dst_ref=sums.at[pl.ds(0, 15)],
            send_sem=sum_send.at[n],
            recv_sem=sum_recv.at[n],
            device_id=(device(0, 0, 1 - core), column),
            device_id_type=MESH,
        )

    def grand(sums, tiles):
        total = [sums[0, n] for n in range(len(tiles))]
        for other in range(1, 16):
            total = [t + sums[other, n] for n, t in enumerate(total)]
        for j, t in zip(tiles, total):
            scale = jnp.sqrt(t)
            if j < 7:
                scale_query[j : j + 1, :] = scale
            elif j == 7:
                scale_key[...] = scale
            else:
                scale_value[...] = scale
            inverse[j] = 1.0 / scale

    late, early = tuple(range(7)), (7, 8)

    loaded(pieces, BLOCK, 512)
    for n, t in enumerate(mix(0, BLOCK, early, zeros(2))):
        sums_early[me, n] = jnp.sum(t, axis=0, keepdims=True)

    @pl.when(jnp.logical_not(at_gate))
    def _():
        pl.semaphore_wait(barrier, 15)

    @pl.when(me == GATE - 1)
    def _():
        pl.semaphore_signal(entered, inc=1, device_id=(GATE, column), device_id_type=MESH)

    @pl.when(at_gate)
    def _():
        pl.semaphore_wait(entered, 1)

    for to in others:
        send_sum(sums_early, 0, *to).start()
    total = zeros(7)
    for piece in range(pieces):
        loaded(piece, 2 * PIECE, 896)
        total = mix(piece * PIECE, PIECE, late, total)
    for n, t in enumerate(total):
        sums_late[me, n] = jnp.sum(t, axis=0, keepdims=True)
    for to in others:
        send_sum(sums_late, 1, *to).start()

    pltpu.make_async_copy(gains, gains, small_sem.at[1]).wait()
    gain_tile[...] = jnp.zeros_like(gain_tile)
    gain_tile[0:1, 0:56] = (gains[0] + gains[1]).astype(jnp.bfloat16).astype(jnp.float32)
    place = lax.rem(56 * (lax.rem(me, 2) * 8 + column), 128)
    gain_rows[column, me] = pltpu.roll(gain_tile[...], place, 1)[0:1, :]

    def send_row():
        return pltpu.make_async_remote_copy(
            src_ref=gain_rows.at[column, me],
            dst_ref=gain_rows.at[column, me],
            send_sem=row_sem.at[0],
            recv_sem=row_sem.at[1],
            device_id=(GATE, column),
            device_id_type=MESH,
        )

    def all_rows():
        return pltpu.make_async_remote_copy(
            src_ref=gain_rows.at[column, pl.ds(0, 15)],
            dst_ref=gain_rows.at[column, pl.ds(0, 15)],
            send_sem=row_sem.at[0],
            recv_sem=row_sem.at[1],
            device_id=(GATE - 1, column),
            device_id_type=MESH,
        )

    def send_group(k):
        return pltpu.make_async_remote_copy(
            src_ref=gain_rows.at[column],
            dst_ref=gain_rows.at[column],
            send_sem=gate_sem.at[0],
            recv_sem=gate_sem.at[1],
            device_id=(GATE, lax.rem(column + k, 8)),
            device_id_type=MESH,
        )

    def all_groups():
        return pltpu.make_async_remote_copy(
            src_ref=gain_rows.at[pl.ds(0, 7)],
            dst_ref=gain_rows.at[pl.ds(0, 7)],
            send_sem=gate_sem.at[0],
            recv_sem=gate_sem.at[1],
            device_id=(GATE - 1, column),
            device_id_type=MESH,
        )

    def send_gain(to):
        return pltpu.make_async_remote_copy(
            src_ref=gain,
            dst_ref=gain,
            send_sem=gain_sem.at[0],
            recv_sem=gain_sem.at[1],
            device_id=(to, column),
            device_id_type=MESH,
        )

    def compose():
        lane = lax.broadcasted_iota(jnp.int32, (1, 128), 1)
        for group in range(8):
            rows = [jnp.zeros((1, 128), jnp.float32) for _ in range(8)]
            for j in range(16):
                values = gain_rows[j % 8, group * 2 + j // 8]
                row, at = (56 * j) // 128, (56 * j) % 128
                rows[row] = jnp.where((lane >= at) & (lane < at + 56), values, rows[row])
                if at + 56 > 128:
                    rows[row + 1] = jnp.where(lane < at + 56 - 128, values, rows[row + 1])
            for row in range(7):
                gain_flat[group * 7 + row : group * 7 + row + 1, :] = rows[row]
        gain[...] = gain_flat[...].astype(jnp.bfloat16)

    spread = [to for to in range(16) if to % 2 == GATE % 2 and to != GATE] + [GATE - 1]

    def place_of(item, on):
        dy, dz, (low, high), (left, width) = item
        start = pl.multiple_of(device(dy, dz, on) * BLOCK + low, 8)
        return (pl.ds(start, high - low), pl.ds(left, width))

    def link_copy(link, step, item):
        place = place_of(item, core)
        sy, sz = SHIFT[link]
        return pltpu.make_async_remote_copy(
            src_ref=gathered.at[place],
            dst_ref=gathered.at[place],
            send_sem=link_send.at[link, step % AHEAD],
            recv_sem=link_recv.at[link, step % SLOTS],
            device_id=(device(sy, sz, core), column),
            device_id_type=MESH,
        )

    def core_copy(place):
        return pltpu.make_async_remote_copy(
            src_ref=gathered.at[place],
            dst_ref=gathered.at[place],
            send_sem=core_send,
            recv_sem=core_recv,
            device_id=(device(0, 0, 1 - core), column),
            device_id_type=MESH,
        )

    def normalise(tiles):
        def body(i, _):
            at = pl.multiple_of(i * 16, 16)
            to = pl.multiple_of(me * BLOCK + i * 16, 16)
            for j in tiles:
                lanes = slice(j * 128, (j + 1) * 128)
                gathered[pl.ds(to, 16), lanes] = (first[pl.ds(at, 16), lanes] * inverse[j]).astype(jnp.bfloat16)
            return 0

        lax.fori_loop(0, BLOCK // 16, body, 0)

    arrived = set()

    def receive(link, step):
        if (link, step) in arrived:
            return
        arrived.add((link, step))
        item = arriving(link, step)
        link_copy(link, step, item).wait_recv()
        core_copy(place_of(item, core)).start()

    all_sums(sums_early, 0).wait_recv()
    grand(sums_early, early)
    normalise(early)

    for step in range(STEPS):
        for link in range(3):
            if step >= AHEAD:
                link_copy(link, step - AHEAD, SENT[link][step - AHEAD]).wait_send()
            item = SENT[link][step]
            if item[:2] != (0, 0):
                for arrival in needed(item):
                    receive(*arrival)
            link_copy(link, step, item).start()
        if step == 0:

            @pl.when(jnp.logical_not(at_gate))
            def _():
                send_row().start()

            all_sums(sums_late, 1).wait_recv()
            grand(sums_late, late)
            normalise(late)
        if step in (1, 2):
            core_copy(place_of((0, 0, ((step - 1) * HALF, step * HALF), ALL), core)).start()
        if step == GAIN_STEPS[0]:

            @pl.when(at_gate)
            def _():
                all_rows().wait_recv()
                pl.semaphore_wait(barrier, 7)
                for k in range(1, 8):
                    send_group(k).start()

        if step == GAIN_STEPS[1]:

            @pl.when(at_gate)
            def _():
                all_groups().wait_recv()
                compose()

        if step == GAIN_STEPS[2]:

            @pl.when(at_gate)
            def _():
                for to in spread:
                    send_gain(to).start()

        if step == GAIN_STEPS[3]:

            @pl.when(jnp.logical_and(jnp.logical_not(at_gate), core == GATE % 2))
            def _():
                send_gain(me).wait_recv()
                send_gain(device(0, 0, 1 - core)).start()

        if step >= AHEAD:
            for link in range(3):
                receive(link, step - AHEAD)

    for step in range(STEPS - AHEAD, STEPS):
        for link in range(3):
            receive(link, step)
    for step in range(STEPS - AHEAD, STEPS):
        for link in range(3):
            link_copy(link, step, SENT[link][step]).wait_send()
    all_sums(sums_early, 0).wait_send()
    all_sums(sums_late, 1).wait_send()

    @pl.when(core != GATE % 2)
    def _():
        send_gain(me).wait_recv()

    @pl.when(at_gate)
    def _():
        all_groups().wait_send()
        gains_sent = gathered.at[pl.ds(0, 448), pl.ds(0, 128)]
        pltpu.make_async_copy(gains_sent, gains_sent, gain_sem.at[0]).wait()

    @pl.when(jnp.logical_not(at_gate))
    def _():
        send_row().wait_send()

        @pl.when(core == GATE % 2)
        def _():
            send_gain(me).wait_send()

    half = core_copy((pl.ds(0, 8 * BLOCK), pl.ds(0, 1152)))
    half.wait_send()
    half.wait_recv()


def write_kernel(gathered, *rest):
    small, (query, key, value), outs, sem = rest[:4], rest[4:7], rest[7:11], rest[11]
    parts = 4
    rows = gathered.shape[0] // parts
    for part in range(parts):
        at = pl.ds(part * rows, rows)
        pltpu.make_async_copy(gathered.at[at, pl.ds(0, 896)], query.at[at, :], sem.at[0]).start()
    others = [
        pltpu.make_async_copy(gathered.at[:, pl.ds(896, 128)], key, sem.at[1]),
        pltpu.make_async_copy(gathered.at[:, pl.ds(1024, 128)], value, sem.at[2]),
    ]
    for source, target in zip(small, outs):
        others.append(pltpu.make_async_copy(source, target, sem.at[len(others) + 1]))
    for copy in others:
        copy.start()
    pltpu.make_async_copy(gathered.at[:, pl.ds(0, 896)], query, sem.at[0]).wait()
    for copy in others:
        copy.wait()


def shards(
    one_query,
    other_query,
    one_key,
    other_key,
    one_value,
    other_value,
    mix_share,
    norm_train,
    norm_step,
):
    dma = pltpu.SemaphoreType.DMA
    f32, bf16 = jnp.float32, jnp.bfloat16
    inputs = [
        pltpu.with_memory_space_constraint(x, HBM)
        for x in (
            one_query,
            other_query,
            one_key,
            other_key,
            one_value,
            other_value,
            mix_share.reshape(1, 448),
            norm_train.reshape(1, 56),
            norm_step.reshape(1, 56),
        )
    ]
    small = (
        jax.ShapeDtypeStruct((7, 128), f32),
        jax.ShapeDtypeStruct((1, 128), f32),
        jax.ShapeDtypeStruct((1, 128), f32),
        jax.ShapeDtypeStruct((56, 128), bf16),
    )
    gathered, *rest = pl.pallas_call(
        gather_kernel,
        out_shape=(jax.ShapeDtypeStruct((7168, 1152), bf16), *small),
        in_specs=[pl.BlockSpec(memory_space=HBM)] * 9,
        out_specs=(pl.BlockSpec(memory_space=VMEM),) * 5,
        scratch_shapes=[
            pltpu.VMEM((448, 1152), f32),
            pltpu.VMEM((448, 1152), f32),
            pltpu.VMEM((1, 448), f32),
            pltpu.VMEM((2, 1, 56), f32),
            pltpu.VMEM((1, 512), f32),
            pltpu.VMEM((512, 128), f32),
            pltpu.VMEM((16, 7, 1, 128), f32),
            pltpu.VMEM((16, 2, 1, 128), f32),
            pltpu.VMEM((9, 1, 128), f32),
            pltpu.VMEM((8, 128), f32),
            pltpu.VMEM((8, 16, 1, 128), f32),
            pltpu.VMEM((56, 128), f32),
            dma((BLOCK // PIECE + 1,)),
            dma((2,)),
            pltpu.SemaphoreType.REGULAR,
            dma((2,)),
            dma((2,)),
            dma((2,)),
            dma((2,)),
            dma((2,)),
            dma((3, AHEAD)),
            dma((3, SLOTS)),
            dma,
            dma,
        ],
        compiler_params=pltpu.CompilerParams(
            collective_id=0, has_side_effects=True, vmem_limit_bytes=32 << 20
        ),
    )(*inputs)
    query, key, value, *outs = pl.pallas_call(
        write_kernel,
        out_shape=(
            jax.ShapeDtypeStruct((7168, 896), bf16),
            jax.ShapeDtypeStruct((7168, 128), bf16),
            jax.ShapeDtypeStruct((7168, 128), bf16),
            *small,
        ),
        in_specs=[pl.BlockSpec(memory_space=VMEM)] * 5,
        out_specs=(pl.BlockSpec(memory_space=HBM),) * 7,
        scratch_shapes=[dma((7,))],
        compiler_params=pltpu.CompilerParams(vmem_limit_bytes=20 << 20),
    )(gathered, *rest)
    return (query, key, value, *(x.reshape(-1) for x in outs))


def solution(mesh):
    in_specs = (
        P("rows", "width"),
        P("rows", "width"),
        P("rows", "width"),
        P("rows", "width"),
        P("rows", "width"),
        P("rows", "width"),
        P("rows"),
        P(("rows", "width")),
        P(("rows", "width")),
    )
    out_specs = (
        P(None, "width"),
        P(None, "width"),
        P(None, "width"),
        P("width"),
        P("width"),
        P("width"),
        P(),
    )
    return jax.shard_map(shards, mesh=mesh, in_specs=in_specs, out_specs=out_specs, check_vma=False)
```

```python
import functools

import jax
import jax.numpy as jnp
from jax import lax
from jax.experimental import pallas as pl
from jax.experimental.pallas import tpu as pltpu
from jax.sharding import PartitionSpec as P

MESH = pl.DeviceIdType.MESH
HBM = pltpu.MemorySpace.HBM
VMEM = pltpu.MemorySpace.VMEM

BLOCK = 448
HALF = 224
PIECE = 112
QUERY = (0, 896)
KEYVALUE = (896, 256)
ALL = (0, 1152)
EARLY = 32
LOW = ((EARLY, 96), (96, 160), (160, 224))
HIGH = ((224, 304), (304, 368), (368, 448))


def own(*parts):
    return [(0, 0, rows, columns) for rows, columns in parts]


def relay(dy, dz, *rows):
    return [(dy, dz, r, ALL) for r in rows]


UP = (
    own(((EARLY, 160), KEYVALUE), (LOW[0], QUERY), (LOW[1], QUERY), (LOW[2], ALL), *((r, ALL) for r in HIGH))
    + relay(-1, 0, (0, 96), *LOW[1:])
    + relay(0, 1, (224, 304), (304, 376))
    + relay(-1, 1, (0, 96), (96, 160), (160, 208), (208, 224))
)
DOWN = (
    own(((224, 368), KEYVALUE), (HIGH[0], QUERY), (HIGH[1], QUERY), (HIGH[2], ALL), *((r, ALL) for r in LOW))
    + relay(1, 0, *HIGH)
    + relay(0, 1, (0, 80), (80, 152))
    + relay(1, 1, (224, 304), (304, 368), (368, 432), (432, 448))
)
ACROSS = (
    own(
        ((EARLY, 160), KEYVALUE),
        (LOW[0], QUERY),
        (HIGH[0], ALL),
        (LOW[1], QUERY),
        (HIGH[1], ALL),
        (LOW[2], ALL),
        (HIGH[2], ALL),
    )
    + relay(-1, 0, (0, 96))
    + relay(1, 0, HIGH[0])
    + relay(-1, 0, LOW[1])
    + relay(1, 0, HIGH[1])
    + relay(-1, 0, LOW[2])
    + relay(1, 0, HIGH[2])
    + relay(-1, 0, (376, 448))
    + relay(1, 0, (152, 208), (208, 224))
)
SENT = (UP, DOWN, ACROSS)
SHIFT = ((1, 0), (-1, 0), (0, 1))
STEPS = len(UP)
AHEAD = 2
SLOTS = 2 * AHEAD + 2
GATE = 5
GAIN_STEPS = (5, 8, 9, 12)
FARTHEST = ((2, 1), (1, 1), (3, 1), (2, 0), (1, 0), (3, 0), (0, 1), (0, 0))


def arriving(link, step):
    dy, dz, rows, columns = SENT[link][step]
    sy, sz = SHIFT[link]
    return ((dy - sy) % 4, (dz - sz) % 2, rows, columns)


ARRIVALS = [(l, s) for s in range(STEPS) for l in range(3)]


def needed(item):
    dy, dz, rows, _ = item
    for l, s in ARRIVALS:
        ay, az, have, _ = arriving(l, s)
        if (ay, az) == (dy % 4, dz % 2) and have[0] < rows[1] and rows[0] < have[1]:
            yield l, s


def gather_kernel(
    one_query,
    other_query,
    one_key,
    other_key,
    one_value,
    other_value,
    share_input,
    train_input,
    step_input,
    gathered,
    scale_query,
    scale_key,
    scale_value,
    gain,
    first,
    second,
    share,
    gains,
    share_row,
    share_tile,
    sums_late,
    sums_early,
    inverse,
    gain_tile,
    gain_rows,
    gain_flat,
    early_rows,
    load_sem,
    small_sem,
    entered,
    sum_send,
    sum_recv,
    row_sem,
    gate_sem,
    gain_sem,
    link_send,
    link_recv,
    core_send,
    core_recv,
    early_sem,
):
    me = lax.axis_index("rows")
    column = lax.axis_index("width")
    core = lax.rem(me, 2)
    y = lax.rem(me // 2, 4)
    z = me // 8

    def device(dy, dz, on):
        return lax.rem(z + dz + 2, 2) * 8 + lax.rem(y + dy + 4, 4) * 2 + on

    at_gate = me == GATE
    barrier = pltpu.get_barrier_semaphore()
    others = [(dy, dz, on) for dy, dz in FARTHEST for on in (0, 1) if (dy, dz, on) != (0, 0, 0)]
    for dy, dz, on in others:
        peer = device(dy, dz, lax.rem(core + on, 2))

        @pl.when(peer != GATE)
        def _():
            pl.semaphore_signal(barrier, inc=1, device_id=(peer, column), device_id_type=MESH)

    @pl.when(at_gate)
    def _():
        for k in range(1, 8):
            pl.semaphore_signal(barrier, inc=1, device_id=(me, lax.rem(column + k, 8)), device_id_type=MESH)

    small = [
        pltpu.make_async_copy(share_input, share, small_sem.at[0]),
        pltpu.make_async_copy(train_input, gains.at[0], small_sem.at[1]),
        pltpu.make_async_copy(step_input, gains.at[1], small_sem.at[1]),
    ]
    pieces = BLOCK // PIECE
    small[0].start()
    for source, target, at in (
        (one_key, first, 896),
        (other_key, second, 896),
        (one_value, first, 1024),
        (other_value, second, 1024),
    ):
        pltpu.make_async_copy(source, target.at[:, pl.ds(at, 128)], load_sem.at[pieces]).start()
    for piece in range(pieces):
        rows = pl.ds(piece * PIECE, PIECE)
        for source, target in ((one_query, first), (other_query, second)):
            pltpu.make_async_copy(source.at[rows, :], target.at[rows, pl.ds(0, 896)], load_sem.at[piece]).start()
    for copy in small[1:]:
        copy.start()

    def loaded(number, rows, columns):
        place = (pl.ds(0, rows), pl.ds(0, columns))
        pltpu.make_async_copy(first.at[place], second.at[place], load_sem.at[number]).wait()

    small[0].wait()
    share_row[...] = jnp.zeros_like(share_row)
    share_row[:, 0:BLOCK] = share[...]
    for part in range(4):
        lanes = share_row[:, part * 128 : (part + 1) * 128]
        share_tile[pl.ds(part * 128, 128), :] = jnp.transpose(jnp.broadcast_to(lanes, (128, 128)))

    def mix(start, rows, tiles, total):
        def body(i, total):
            total = list(total)
            for part in range(2):
                at = pl.ds(pl.multiple_of(start + i * 16 + part * 8, 8), 8)
                mine = share_tile[at, :]
                rest = 1.0 - mine
                for n, j in enumerate(tiles):
                    lanes = slice(j * 128, (j + 1) * 128)
                    result = mine * first[at, lanes] + rest * second[at, lanes]
                    first[at, lanes] = result
                    total[n] = total[n] + result * result
            return tuple(total)

        return lax.fori_loop(0, rows // 16, body, total, unroll=2 if len(tiles) == 2 else 1)

    def zeros(n):
        return tuple(jnp.zeros((8, 128), jnp.float32) for _ in range(n))

    def send_sum(sums, n, dy, dz, on):
        return pltpu.make_async_remote_copy(
            src_ref=sums.at[me],
            dst_ref=sums.at[me],
            send_sem=sum_send.at[n],
            recv_sem=sum_recv.at[n],
            device_id=(device(dy, dz, lax.rem(core + on, 2)), column),
            device_id_type=MESH,
        )

    def all_sums(sums, n):
        return pltpu.make_async_remote_copy(
            src_ref=sums.at[pl.ds(0, 15)],
            dst_ref=sums.at[pl.ds(0, 15)],
            send_sem=sum_send.at[n],
            recv_sem=sum_recv.at[n],
            device_id=(device(0, 0, 1 - core), column),
            device_id_type=MESH,
        )

    def grand(sums, tiles):
        total = [sums[0, n] for n in range(len(tiles))]
        for other in range(1, 16):
            total = [t + sums[other, n] for n, t in enumerate(total)]
        for j, t in zip(tiles, total):
            scale = jnp.sqrt(t)
            if j < 7:
                scale_query[j : j + 1, :] = scale
            elif j == 7:
                scale_key[...] = scale
            else:
                scale_value[...] = scale
            inverse[j] = 1.0 / scale

    late, early = tuple(range(7)), (7, 8)

    loaded(pieces, BLOCK, 512)
    for n, t in enumerate(mix(0, BLOCK, early, zeros(2))):
        sums_early[me, n] = jnp.sum(t, axis=0, keepdims=True)

    @pl.when(jnp.logical_not(at_gate))
    def _():
        pl.semaphore_wait(barrier, 15)

    @pl.when(me == GATE - 1)
    def _():
        pl.semaphore_signal(entered, inc=1, device_id=(GATE, column), device_id_type=MESH)

    @pl.when(at_gate)
    def _():
        pl.semaphore_wait(entered, 1)

    for to in others:
        send_sum(sums_early, 0, *to).start()
    total = zeros(7)
    for piece in range(pieces):
        loaded(piece, 2 * PIECE, 896)
        total = mix(piece * PIECE, PIECE, late, total)
    for n, t in enumerate(total):
        sums_late[me, n] = jnp.sum(t, axis=0, keepdims=True)
    for to in others:
        send_sum(sums_late, 1, *to).start()

    def early_copy(link):
        sy, sz = SHIFT[link]
        return pltpu.make_async_remote_copy(
            src_ref=first.at[pl.ds(0, EARLY), :],
            dst_ref=early_rows.at[link],
            send_sem=early_sem.at[0],
            recv_sem=early_sem.at[1],
            device_id=(device(sy, sz, core), column),
            device_id_type=MESH,
        )

    def all_early():
        return pltpu.make_async_remote_copy(
            src_ref=early_rows,
            dst_ref=early_rows,
            send_sem=early_sem.at[0],
            recv_sem=early_sem.at[1],
            device_id=(device(0, 0, 1 - core), column),
            device_id_type=MESH,
        )

    for link in range(3):
        early_copy(link).start()

    pltpu.make_async_copy(gains, gains, small_sem.at[1]).wait()
    gain_tile[...] = jnp.zeros_like(gain_tile)
    gain_tile[0:1, 0:56] = (gains[0] + gains[1]).astype(jnp.bfloat16).astype(jnp.float32)
    place = lax.rem(56 * (lax.rem(me, 2) * 8 + column), 128)
    gain_rows[column, me] = pltpu.roll(gain_tile[...], place, 1)[0:1, :]

    def send_row():
        return pltpu.make_async_remote_copy(
            src_ref=gain_rows.at[column, me],
            dst_ref=gain_rows.at[column, me],
            send_sem=row_sem.at[0],
            recv_sem=row_sem.at[1],
            device_id=(GATE, column),
            device_id_type=MESH,
        )

    def all_rows():
        return pltpu.make_async_remote_copy(
            src_ref=gain_rows.at[column, pl.ds(0, 15)],
            dst_ref=gain_rows.at[column, pl.ds(0, 15)],
            send_sem=row_sem.at[0],
            recv_sem=row_sem.at[1],
            device_id=(GATE - 1, column),
            device_id_type=MESH,
        )

    def send_group(k):
        return pltpu.make_async_remote_copy(
            src_ref=gain_rows.at[column],
            dst_ref=gain_rows.at[column],
            send_sem=gate_sem.at[0],
            recv_sem=gate_sem.at[1],
            device_id=(GATE, lax.rem(column + k, 8)),
            device_id_type=MESH,
        )

    def all_groups():
        return pltpu.make_async_remote_copy(
            src_ref=gain_rows.at[pl.ds(0, 7)],
            dst_ref=gain_rows.at[pl.ds(0, 7)],
            send_sem=gate_sem.at[0],
            recv_sem=gate_sem.at[1],
            device_id=(GATE - 1, column),
            device_id_type=MESH,
        )

    def send_gain(to):
        return pltpu.make_async_remote_copy(
            src_ref=gain,
            dst_ref=gain,
            send_sem=gain_sem.at[0],
            recv_sem=gain_sem.at[1],
            device_id=(to, column),
            device_id_type=MESH,
        )

    def compose():
        lane = lax.broadcasted_iota(jnp.int32, (1, 128), 1)
        for group in range(8):
            rows = [jnp.zeros((1, 128), jnp.float32) for _ in range(8)]
            for j in range(16):
                values = gain_rows[j % 8, group * 2 + j // 8]
                row, at = (56 * j) // 128, (56 * j) % 128
                rows[row] = jnp.where((lane >= at) & (lane < at + 56), values, rows[row])
                if at + 56 > 128:
                    rows[row + 1] = jnp.where(lane < at + 56 - 128, values, rows[row + 1])
            for row in range(7):
                gain_flat[group * 7 + row : group * 7 + row + 1, :] = rows[row]
        gain[...] = gain_flat[...].astype(jnp.bfloat16)

    spread = [to for to in range(16) if to % 2 == GATE % 2 and to != GATE] + [GATE - 1]

    def place_of(item, on):
        dy, dz, (low, high), (left, width) = item
        start = pl.multiple_of(device(dy, dz, on) * BLOCK + low, 8)
        return (pl.ds(start, high - low), pl.ds(left, width))

    def link_copy(link, step, item):
        place = place_of(item, core)
        sy, sz = SHIFT[link]
        return pltpu.make_async_remote_copy(
            src_ref=gathered.at[place],
            dst_ref=gathered.at[place],
            send_sem=link_send.at[link, step % AHEAD],
            recv_sem=link_recv.at[link, step % SLOTS],
            device_id=(device(sy, sz, core), column),
            device_id_type=MESH,
        )

    def core_copy(place):
        return pltpu.make_async_remote_copy(
            src_ref=gathered.at[place],
            dst_ref=gathered.at[place],
            send_sem=core_send,
            recv_sem=core_recv,
            device_id=(device(0, 0, 1 - core), column),
            device_id_type=MESH,
        )

    def normalise(tiles):
        def body(i, _):
            at = pl.multiple_of(i * 16, 16)
            to = pl.multiple_of(me * BLOCK + i * 16, 16)
            for j in tiles:
                lanes = slice(j * 128, (j + 1) * 128)
                gathered[pl.ds(to, 16), lanes] = (first[pl.ds(at, 16), lanes] * inverse[j]).astype(jnp.bfloat16)
            return 0

        lax.fori_loop(0, BLOCK // 16, body, 0)

    def normalise_early():
        for link, (sy, sz) in enumerate(SHIFT):
            for i in range(EARLY // 16):
                to = pl.multiple_of(device(-sy, -sz, core) * BLOCK + i * 16, 16)
                for j in range(9):
                    lanes = slice(j * 128, (j + 1) * 128)
                    values = early_rows[link, i * 16 : (i + 1) * 16, lanes] * inverse[j]
                    gathered[pl.ds(to, 16), lanes] = values.astype(jnp.bfloat16)

    arrived = set()

    def receive(link, step):
        if (link, step) in arrived:
            return
        arrived.add((link, step))
        item = arriving(link, step)
        link_copy(link, step, item).wait_recv()
        core_copy(place_of(item, core)).start()

    all_sums(sums_early, 0).wait_recv()
    grand(sums_early, early)
    normalise(early)

    for step in range(STEPS):
        for link in range(3):
            if step >= AHEAD:
                link_copy(link, step - AHEAD, SENT[link][step - AHEAD]).wait_send()
            item = SENT[link][step]
            if item[:2] != (0, 0):
                for arrival in needed(item):
                    receive(*arrival)
            link_copy(link, step, item).start()
        if step == 0:

            @pl.when(jnp.logical_not(at_gate))
            def _():
                send_row().start()

            all_sums(sums_late, 1).wait_recv()
            grand(sums_late, late)
            normalise(late)
        if step == 1:
            all_early().wait_recv()
            normalise_early()
        if step == 3:
            for sy, sz in SHIFT:
                core_copy(place_of((-sy, -sz, (0, EARLY), ALL), core)).start()
        if step in (1, 2):
            core_copy(place_of((0, 0, ((step - 1) * HALF, step * HALF), ALL), core)).start()
        if step == GAIN_STEPS[0]:

            @pl.when(at_gate)
            def _():
                all_rows().wait_recv()
                pl.semaphore_wait(barrier, 7)
                for k in range(1, 8):
                    send_group(k).start()

        if step == GAIN_STEPS[1]:

            @pl.when(at_gate)
            def _():
                all_groups().wait_recv()
                compose()

        if step == GAIN_STEPS[2]:

            @pl.when(at_gate)
            def _():
                for to in spread:
                    send_gain(to).start()

        if step == GAIN_STEPS[3]:

            @pl.when(jnp.logical_and(jnp.logical_not(at_gate), core == GATE % 2))
            def _():
                send_gain(me).wait_recv()
                send_gain(device(0, 0, 1 - core)).start()

        if step >= AHEAD:
            for link in range(3):
                receive(link, step - AHEAD)

    for step in range(STEPS - AHEAD, STEPS):
        for link in range(3):
            receive(link, step)
    for step in range(STEPS - AHEAD, STEPS):
        for link in range(3):
            link_copy(link, step, SENT[link][step]).wait_send()
    all_early().wait_send()
    all_sums(sums_early, 0).wait_send()
    all_sums(sums_late, 1).wait_send()

    @pl.when(core != GATE % 2)
    def _():
        send_gain(me).wait_recv()

    @pl.when(at_gate)
    def _():
        all_groups().wait_send()
        gains_sent = gathered.at[pl.ds(0, 448), pl.ds(0, 128)]
        pltpu.make_async_copy(gains_sent, gains_sent, gain_sem.at[0]).wait()

    @pl.when(jnp.logical_not(at_gate))
    def _():
        send_row().wait_send()

        @pl.when(core == GATE % 2)
        def _():
            send_gain(me).wait_send()

    half = core_copy((pl.ds(0, 8 * BLOCK), pl.ds(0, 1152)))
    half.wait_send()
    half.wait_recv()


def write_kernel(gathered, *rest):
    small, (query, key, value), outs, sem = rest[:4], rest[4:7], rest[7:11], rest[11]
    parts = 4
    rows = gathered.shape[0] // parts
    for part in range(parts):
        at = pl.ds(part * rows, rows)
        pltpu.make_async_copy(gathered.at[at, pl.ds(0, 896)], query.at[at, :], sem.at[0]).start()
    others = [
        pltpu.make_async_copy(gathered.at[:, pl.ds(896, 128)], key, sem.at[1]),
        pltpu.make_async_copy(gathered.at[:, pl.ds(1024, 128)], value, sem.at[2]),
    ]
    for source, target in zip(small, outs):
        others.append(pltpu.make_async_copy(source, target, sem.at[len(others) + 1]))
    for copy in others:
        copy.start()
    pltpu.make_async_copy(gathered.at[:, pl.ds(0, 896)], query, sem.at[0]).wait()
    for copy in others:
        copy.wait()


def shards(
    one_query,
    other_query,
    one_key,
    other_key,
    one_value,
    other_value,
    mix_share,
    norm_train,
    norm_step,
):
    dma = pltpu.SemaphoreType.DMA
    f32, bf16 = jnp.float32, jnp.bfloat16
    inputs = [
        pltpu.with_memory_space_constraint(x, HBM)
        for x in (
            one_query,
            other_query,
            one_key,
            other_key,
            one_value,
            other_value,
            mix_share.reshape(1, 448),
            norm_train.reshape(1, 56),
            norm_step.reshape(1, 56),
        )
    ]
    small = (
        jax.ShapeDtypeStruct((7, 128), f32),
        jax.ShapeDtypeStruct((1, 128), f32),
        jax.ShapeDtypeStruct((1, 128), f32),
        jax.ShapeDtypeStruct((56, 128), bf16),
    )
    gathered, *rest = pl.pallas_call(
        gather_kernel,
        out_shape=(jax.ShapeDtypeStruct((7168, 1152), bf16), *small),
        in_specs=[pl.BlockSpec(memory_space=HBM)] * 9,
        out_specs=(pl.BlockSpec(memory_space=VMEM),) * 5,
        scratch_shapes=[
            pltpu.VMEM((448, 1152), f32),
            pltpu.VMEM((448, 1152), f32),
            pltpu.VMEM((1, 448), f32),
            pltpu.VMEM((2, 1, 56), f32),
            pltpu.VMEM((1, 512), f32),
            pltpu.VMEM((512, 128), f32),
            pltpu.VMEM((16, 7, 1, 128), f32),
            pltpu.VMEM((16, 2, 1, 128), f32),
            pltpu.VMEM((9, 1, 128), f32),
            pltpu.VMEM((8, 128), f32),
            pltpu.VMEM((8, 16, 1, 128), f32),
            pltpu.VMEM((56, 128), f32),
            pltpu.VMEM((3, EARLY, 1152), f32),
            dma((BLOCK // PIECE + 1,)),
            dma((2,)),
            pltpu.SemaphoreType.REGULAR,
            dma((2,)),
            dma((2,)),
            dma((2,)),
            dma((2,)),
            dma((2,)),
            dma((3, AHEAD)),
            dma((3, SLOTS)),
            dma,
            dma,
            dma((2,)),
        ],
        compiler_params=pltpu.CompilerParams(
            collective_id=0, has_side_effects=True, vmem_limit_bytes=32 << 20
        ),
    )(*inputs)
    query, key, value, *outs = pl.pallas_call(
        write_kernel,
        out_shape=(
            jax.ShapeDtypeStruct((7168, 896), bf16),
            jax.ShapeDtypeStruct((7168, 128), bf16),
            jax.ShapeDtypeStruct((7168, 128), bf16),
            *small,
        ),
        in_specs=[pl.BlockSpec(memory_space=VMEM)] * 5,
        out_specs=(pl.BlockSpec(memory_space=HBM),) * 7,
        scratch_shapes=[dma((7,))],
        compiler_params=pltpu.CompilerParams(vmem_limit_bytes=20 << 20),
    )(gathered, *rest)
    return (query, key, value, *(x.reshape(-1) for x in outs))


def solution(mesh):
    in_specs = (
        P("rows", "width"),
        P("rows", "width"),
        P("rows", "width"),
        P("rows", "width"),
        P("rows", "width"),
        P("rows", "width"),
        P("rows"),
        P(("rows", "width")),
        P(("rows", "width")),
    )
    out_specs = (
        P(None, "width"),
        P(None, "width"),
        P(None, "width"),
        P("width"),
        P("width"),
        P("width"),
        P(),
    )
    return jax.shard_map(shards, mesh=mesh, in_specs=in_specs, out_specs=out_specs, check_vma=False)
```

```python
import functools

import jax
import jax.numpy as jnp
from jax import lax
from jax.experimental import pallas as pl
from jax.experimental.pallas import tpu as pltpu
from jax.sharding import PartitionSpec as P

MESH = pl.DeviceIdType.MESH
HBM = pltpu.MemorySpace.HBM
VMEM = pltpu.MemorySpace.VMEM

BLOCK = 448
HALF = 224
PIECE = 112
QUERY = (0, 896)
KEYVALUE = (896, 256)
ALL = (0, 1152)
EARLY = 32
LAST = 8
LOW = ((EARLY, 96), (96, 160), (160, 224))
HIGH = ((224, 304), (304, 368), (368, 448))


def own(*parts):
    return [(0, 0, rows, columns) for rows, columns in parts]


def relay(dy, dz, *rows):
    return [(dy, dz, r, ALL) for r in rows]


UP = (
    own(((EARLY, 160), KEYVALUE), (LOW[0], QUERY), (LOW[1], QUERY), (LOW[2], ALL), *((r, ALL) for r in HIGH))
    + relay(-1, 0, (0, 96), *LOW[1:])
    + relay(0, 1, (224, 304), (304, 376))
    + relay(-1, 1, (0, 96), (96, 160), (160, 200), (200, 216), (216, 224))
)
DOWN = (
    own(((224, 368), KEYVALUE), (HIGH[0], QUERY), (HIGH[1], QUERY), (HIGH[2], ALL), *((r, ALL) for r in LOW))
    + relay(1, 0, *HIGH)
    + relay(0, 1, (0, 80), (80, 152))
    + relay(1, 1, (224, 304), (304, 368), (368, 424), (424, 440), (440, 448))
)
ACROSS = (
    own(
        ((EARLY, 160), KEYVALUE),
        (LOW[0], QUERY),
        (HIGH[0], ALL),
        (LOW[1], QUERY),
        (HIGH[1], ALL),
        (LOW[2], ALL),
        (HIGH[2], ALL),
    )
    + relay(-1, 0, (0, 96))
    + relay(1, 0, HIGH[0])
    + relay(-1, 0, LOW[1])
    + relay(1, 0, HIGH[1])
    + relay(-1, 0, LOW[2])
    + relay(1, 0, HIGH[2])
    + relay(-1, 0, (376, 448))
    + relay(1, 0, (152, 200), (200, 216), (216, 224))
)
SENT = (UP, DOWN, ACROSS)
SHIFT = ((1, 0), (-1, 0), (0, 1))
STEPS = len(UP)
AHEAD = 2
SLOTS = 2 * AHEAD + 2
GATE = 5
GAIN_STEPS = (5, 8, 9, 12)
FARTHEST = ((2, 1), (1, 1), (3, 1), (2, 0), (1, 0), (3, 0), (0, 1), (0, 0))


def arriving(link, step):
    dy, dz, rows, columns = SENT[link][step]
    sy, sz = SHIFT[link]
    return ((dy - sy) % 4, (dz - sz) % 2, rows, columns)


ARRIVALS = [(l, s) for s in range(STEPS) for l in range(3)]


def needed(item):
    dy, dz, rows, _ = item
    for l, s in ARRIVALS:
        ay, az, have, _ = arriving(l, s)
        if (ay, az) == (dy % 4, dz % 2) and have[0] < rows[1] and rows[0] < have[1]:
            yield l, s


def gather_kernel(
    one_query,
    other_query,
    one_key,
    other_key,
    one_value,
    other_value,
    share_input,
    train_input,
    step_input,
    gathered,
    scale_query,
    scale_key,
    scale_value,
    gain,
    first,
    second,
    share,
    gains,
    share_row,
    share_tile,
    sums_late,
    sums_early,
    inverse,
    gain_tile,
    gain_rows,
    gain_flat,
    early_rows,
    load_sem,
    small_sem,
    entered,
    sum_send,
    sum_recv,
    row_sem,
    gate_sem,
    gain_sem,
    link_send,
    link_recv,
    core_send,
    core_recv,
    early_sem,
    last_sem,
):
    me = lax.axis_index("rows")
    column = lax.axis_index("width")
    core = lax.rem(me, 2)
    y = lax.rem(me // 2, 4)
    z = me // 8

    def device(dy, dz, on):
        return lax.rem(z + dz + 2, 2) * 8 + lax.rem(y + dy + 4, 4) * 2 + on

    at_gate = me == GATE
    barrier = pltpu.get_barrier_semaphore()
    others = [(dy, dz, on) for dy, dz in FARTHEST for on in (0, 1) if (dy, dz, on) != (0, 0, 0)]
    for dy, dz, on in others:
        peer = device(dy, dz, lax.rem(core + on, 2))

        @pl.when(peer != GATE)
        def _():
            pl.semaphore_signal(barrier, inc=1, device_id=(peer, column), device_id_type=MESH)

    @pl.when(at_gate)
    def _():
        for k in range(1, 8):
            pl.semaphore_signal(barrier, inc=1, device_id=(me, lax.rem(column + k, 8)), device_id_type=MESH)

    small = [
        pltpu.make_async_copy(share_input, share, small_sem.at[0]),
        pltpu.make_async_copy(train_input, gains.at[0], small_sem.at[1]),
        pltpu.make_async_copy(step_input, gains.at[1], small_sem.at[1]),
    ]
    pieces = BLOCK // PIECE
    small[0].start()
    for source, target, at in (
        (one_key, first, 896),
        (other_key, second, 896),
        (one_value, first, 1024),
        (other_value, second, 1024),
    ):
        pltpu.make_async_copy(source, target.at[:, pl.ds(at, 128)], load_sem.at[pieces]).start()
    for piece in range(pieces):
        rows = pl.ds(piece * PIECE, PIECE)
        for source, target in ((one_query, first), (other_query, second)):
            pltpu.make_async_copy(source.at[rows, :], target.at[rows, pl.ds(0, 896)], load_sem.at[piece]).start()
    for copy in small[1:]:
        copy.start()

    def loaded(number, rows, columns):
        place = (pl.ds(0, rows), pl.ds(0, columns))
        pltpu.make_async_copy(first.at[place], second.at[place], load_sem.at[number]).wait()

    small[0].wait()
    share_row[...] = jnp.zeros_like(share_row)
    share_row[:, 0:BLOCK] = share[...]
    for part in range(4):
        lanes = share_row[:, part * 128 : (part + 1) * 128]
        share_tile[pl.ds(part * 128, 128), :] = jnp.transpose(jnp.broadcast_to(lanes, (128, 128)))

    def mix(start, rows, tiles, total):
        def body(i, total):
            total = list(total)
            for part in range(2):
                at = pl.ds(pl.multiple_of(start + i * 16 + part * 8, 8), 8)
                mine = share_tile[at, :]
                rest = 1.0 - mine
                for n, j in enumerate(tiles):
                    lanes = slice(j * 128, (j + 1) * 128)
                    result = mine * first[at, lanes] + rest * second[at, lanes]
                    first[at, lanes] = result
                    total[n] = total[n] + result * result
            return tuple(total)

        return lax.fori_loop(0, rows // 16, body, total, unroll=2 if len(tiles) == 2 else 1)

    def zeros(n):
        return tuple(jnp.zeros((8, 128), jnp.float32) for _ in range(n))

    def send_sum(sums, n, dy, dz, on):
        return pltpu.make_async_remote_copy(
            src_ref=sums.at[me],
            dst_ref=sums.at[me],
            send_sem=sum_send.at[n],
            recv_sem=sum_recv.at[n],
            device_id=(device(dy, dz, lax.rem(core + on, 2)), column),
            device_id_type=MESH,
        )

    def all_sums(sums, n):
        return pltpu.make_async_remote_copy(
            src_ref=sums.at[pl.ds(0, 15)],
            dst_ref=sums.at[pl.ds(0, 15)],
            send_sem=sum_send.at[n],
            recv_sem=sum_recv.at[n],
            device_id=(device(0, 0, 1 - core), column),
            device_id_type=MESH,
        )

    def grand(sums, tiles):
        total = [sums[0, n] for n in range(len(tiles))]
        for other in range(1, 16):
            total = [t + sums[other, n] for n, t in enumerate(total)]
        for j, t in zip(tiles, total):
            scale = jnp.sqrt(t)
            if j < 7:
                scale_query[j : j + 1, :] = scale
            elif j == 7:
                scale_key[...] = scale
            else:
                scale_value[...] = scale
            inverse[j] = 1.0 / scale

    late, early = tuple(range(7)), (7, 8)

    loaded(pieces, BLOCK, 512)
    for n, t in enumerate(mix(0, BLOCK, early, zeros(2))):
        sums_early[me, n] = jnp.sum(t, axis=0, keepdims=True)

    @pl.when(jnp.logical_not(at_gate))
    def _():
        pl.semaphore_wait(barrier, 15)

    @pl.when(me == GATE - 1)
    def _():
        pl.semaphore_signal(entered, inc=1, device_id=(GATE, column), device_id_type=MESH)

    @pl.when(at_gate)
    def _():
        pl.semaphore_wait(entered, 1)

    for to in others:
        send_sum(sums_early, 0, *to).start()
    total = zeros(7)
    for piece in range(pieces):
        loaded(piece, 2 * PIECE, 896)
        total = mix(piece * PIECE, PIECE, late, total)
    for n, t in enumerate(total):
        sums_late[me, n] = jnp.sum(t, axis=0, keepdims=True)
    for to in others:
        send_sum(sums_late, 1, *to).start()

    def early_copy(link):
        sy, sz = SHIFT[link]
        return pltpu.make_async_remote_copy(
            src_ref=first.at[pl.ds(0, EARLY), :],
            dst_ref=early_rows.at[link],
            send_sem=early_sem.at[0],
            recv_sem=early_sem.at[1],
            device_id=(device(sy, sz, core), column),
            device_id_type=MESH,
        )

    def all_early():
        return pltpu.make_async_remote_copy(
            src_ref=early_rows,
            dst_ref=early_rows,
            send_sem=early_sem.at[0],
            recv_sem=early_sem.at[1],
            device_id=(device(0, 0, 1 - core), column),
            device_id_type=MESH,
        )

    for link in range(3):
        early_copy(link).start()

    pltpu.make_async_copy(gains, gains, small_sem.at[1]).wait()
    gain_tile[...] = jnp.zeros_like(gain_tile)
    gain_tile[0:1, 0:56] = (gains[0] + gains[1]).astype(jnp.bfloat16).astype(jnp.float32)
    place = lax.rem(56 * (lax.rem(me, 2) * 8 + column), 128)
    gain_rows[column, me] = pltpu.roll(gain_tile[...], place, 1)[0:1, :]

    def send_row():
        return pltpu.make_async_remote_copy(
            src_ref=gain_rows.at[column, me],
            dst_ref=gain_rows.at[column, me],
            send_sem=row_sem.at[0],
            recv_sem=row_sem.at[1],
            device_id=(GATE, column),
            device_id_type=MESH,
        )

    def all_rows():
        return pltpu.make_async_remote_copy(
            src_ref=gain_rows.at[column, pl.ds(0, 15)],
            dst_ref=gain_rows.at[column, pl.ds(0, 15)],
            send_sem=row_sem.at[0],
            recv_sem=row_sem.at[1],
            device_id=(GATE - 1, column),
            device_id_type=MESH,
        )

    def send_group(k):
        return pltpu.make_async_remote_copy(
            src_ref=gain_rows.at[column],
            dst_ref=gain_rows.at[column],
            send_sem=gate_sem.at[0],
            recv_sem=gate_sem.at[1],
            device_id=(GATE, lax.rem(column + k, 8)),
            device_id_type=MESH,
        )

    def all_groups():
        return pltpu.make_async_remote_copy(
            src_ref=gain_rows.at[pl.ds(0, 7)],
            dst_ref=gain_rows.at[pl.ds(0, 7)],
            send_sem=gate_sem.at[0],
            recv_sem=gate_sem.at[1],
            device_id=(GATE - 1, column),
            device_id_type=MESH,
        )

    def send_gain(to):
        return pltpu.make_async_remote_copy(
            src_ref=gain,
            dst_ref=gain,
            send_sem=gain_sem.at[0],
            recv_sem=gain_sem.at[1],
            device_id=(to, column),
            device_id_type=MESH,
        )

    def compose():
        lane = lax.broadcasted_iota(jnp.int32, (1, 128), 1)
        for group in range(8):
            rows = [jnp.zeros((1, 128), jnp.float32) for _ in range(8)]
            for j in range(16):
                values = gain_rows[j % 8, group * 2 + j // 8]
                row, at = (56 * j) // 128, (56 * j) % 128
                rows[row] = jnp.where((lane >= at) & (lane < at + 56), values, rows[row])
                if at + 56 > 128:
                    rows[row + 1] = jnp.where(lane < at + 56 - 128, values, rows[row + 1])
            for row in range(7):
                gain_flat[group * 7 + row : group * 7 + row + 1, :] = rows[row]
        gain[...] = gain_flat[...].astype(jnp.bfloat16)

    spread = [to for to in range(16) if to % 2 == GATE % 2 and to != GATE] + [GATE - 1]

    def place_of(item, on):
        dy, dz, (low, high), (left, width) = item
        start = pl.multiple_of(device(dy, dz, on) * BLOCK + low, 8)
        return (pl.ds(start, high - low), pl.ds(left, width))

    def link_copy(link, step, item):
        place = place_of(item, core)
        sy, sz = SHIFT[link]
        return pltpu.make_async_remote_copy(
            src_ref=gathered.at[place],
            dst_ref=gathered.at[place],
            send_sem=link_send.at[link, step % AHEAD],
            recv_sem=link_recv.at[link, step % SLOTS],
            device_id=(device(sy, sz, core), column),
            device_id_type=MESH,
        )

    def last_copy(link):
        place = place_of(SENT[link][STEPS - 1], core)
        sy, sz = SHIFT[link]
        return pltpu.make_async_remote_copy(
            src_ref=gathered.at[place],
            dst_ref=gathered.at[place],
            send_sem=last_sem.at[0],
            recv_sem=last_sem.at[1],
            device_id=(device(sy, sz, 1 - core), column),
            device_id_type=MESH,
        )

    def core_copy(place):
        return pltpu.make_async_remote_copy(
            src_ref=gathered.at[place],
            dst_ref=gathered.at[place],
            send_sem=core_send,
            recv_sem=core_recv,
            device_id=(device(0, 0, 1 - core), column),
            device_id_type=MESH,
        )

    def normalise(tiles):
        def body(i, _):
            at = pl.multiple_of(i * 16, 16)
            to = pl.multiple_of(me * BLOCK + i * 16, 16)
            for j in tiles:
                lanes = slice(j * 128, (j + 1) * 128)
                gathered[pl.ds(to, 16), lanes] = (first[pl.ds(at, 16), lanes] * inverse[j]).astype(jnp.bfloat16)
            return 0

        lax.fori_loop(0, BLOCK // 16, body, 0)

    def normalise_early():
        for link, (sy, sz) in enumerate(SHIFT):
            for i in range(EARLY // 16):
                to = pl.multiple_of(device(-sy, -sz, core) * BLOCK + i * 16, 16)
                for j in range(9):
                    lanes = slice(j * 128, (j + 1) * 128)
                    values = early_rows[link, i * 16 : (i + 1) * 16, lanes] * inverse[j]
                    gathered[pl.ds(to, 16), lanes] = values.astype(jnp.bfloat16)

    arrived = set()

    def receive(link, step):
        if (link, step) in arrived:
            return
        arrived.add((link, step))
        item = arriving(link, step)
        link_copy(link, step, item).wait_recv()
        if step < STEPS - 1:
            core_copy(place_of(item, core)).start()

    all_sums(sums_early, 0).wait_recv()
    grand(sums_early, early)
    normalise(early)

    for step in range(STEPS):
        for link in range(3):
            if step >= AHEAD:
                link_copy(link, step - AHEAD, SENT[link][step - AHEAD]).wait_send()
            item = SENT[link][step]
            if item[:2] != (0, 0):
                for arrival in needed(item):
                    receive(*arrival)
            link_copy(link, step, item).start()
            if step == STEPS - 1:
                last_copy(link).start()
        if step == 0:

            @pl.when(jnp.logical_not(at_gate))
            def _():
                send_row().start()

            all_sums(sums_late, 1).wait_recv()
            grand(sums_late, late)
            normalise(late)
        if step == 1:
            all_early().wait_recv()
            normalise_early()
        if step == 3:
            for sy, sz in SHIFT:
                core_copy(place_of((-sy, -sz, (0, EARLY), ALL), core)).start()
        if step in (1, 2):
            core_copy(place_of((0, 0, ((step - 1) * HALF, step * HALF), ALL), core)).start()
        if step == GAIN_STEPS[0]:

            @pl.when(at_gate)
            def _():
                all_rows().wait_recv()
                pl.semaphore_wait(barrier, 7)
                for k in range(1, 8):
                    send_group(k).start()

        if step == GAIN_STEPS[1]:

            @pl.when(at_gate)
            def _():
                all_groups().wait_recv()
                compose()

        if step == GAIN_STEPS[2]:

            @pl.when(at_gate)
            def _():
                for to in spread:
                    send_gain(to).start()

        if step == GAIN_STEPS[3]:

            @pl.when(jnp.logical_and(jnp.logical_not(at_gate), core == GATE % 2))
            def _():
                send_gain(me).wait_recv()
                send_gain(device(0, 0, 1 - core)).start()

        if step >= AHEAD:
            for link in range(3):
                receive(link, step - AHEAD)

    for step in range(STEPS - AHEAD, STEPS):
        for link in range(3):
            receive(link, step)
    for step in range(STEPS - AHEAD, STEPS):
        for link in range(3):
            link_copy(link, step, SENT[link][step]).wait_send()
    all_early().wait_send()
    all_sums(sums_early, 0).wait_send()
    all_sums(sums_late, 1).wait_send()

    @pl.when(core != GATE % 2)
    def _():
        send_gain(me).wait_recv()

    @pl.when(at_gate)
    def _():
        all_groups().wait_send()
        gains_sent = gathered.at[pl.ds(0, 448), pl.ds(0, 128)]
        pltpu.make_async_copy(gains_sent, gains_sent, gain_sem.at[0]).wait()

    @pl.when(jnp.logical_not(at_gate))
    def _():
        send_row().wait_send()

        @pl.when(core == GATE % 2)
        def _():
            send_gain(me).wait_send()

    half = core_copy((pl.ds(0, 8 * BLOCK - 3 * LAST), pl.ds(0, 1152)))
    half.wait_send()
    half.wait_recv()
    rows = gathered.at[pl.ds(0, 3 * LAST), :]
    for n in range(2):
        pltpu.make_async_copy(rows, rows, last_sem.at[n]).wait()


def write_kernel(gathered, *rest):
    small, (query, key, value), outs, sem = rest[:4], rest[4:7], rest[7:11], rest[11]
    parts = 4
    rows = gathered.shape[0] // parts
    for part in range(parts):
        at = pl.ds(part * rows, rows)
        pltpu.make_async_copy(gathered.at[at, pl.ds(0, 896)], query.at[at, :], sem.at[0]).start()
    others = [
        pltpu.make_async_copy(gathered.at[:, pl.ds(896, 128)], key, sem.at[1]),
        pltpu.make_async_copy(gathered.at[:, pl.ds(1024, 128)], value, sem.at[2]),
    ]
    for source, target in zip(small, outs):
        others.append(pltpu.make_async_copy(source, target, sem.at[len(others) + 1]))
    for copy in others:
        copy.start()
    pltpu.make_async_copy(gathered.at[:, pl.ds(0, 896)], query, sem.at[0]).wait()
    for copy in others:
        copy.wait()


def shards(
    one_query,
    other_query,
    one_key,
    other_key,
    one_value,
    other_value,
    mix_share,
    norm_train,
    norm_step,
):
    dma = pltpu.SemaphoreType.DMA
    f32, bf16 = jnp.float32, jnp.bfloat16
    inputs = [
        pltpu.with_memory_space_constraint(x, HBM)
        for x in (
            one_query,
            other_query,
            one_key,
            other_key,
            one_value,
            other_value,
            mix_share.reshape(1, 448),
            norm_train.reshape(1, 56),
            norm_step.reshape(1, 56),
        )
    ]
    small = (
        jax.ShapeDtypeStruct((7, 128), f32),
        jax.ShapeDtypeStruct((1, 128), f32),
        jax.ShapeDtypeStruct((1, 128), f32),
        jax.ShapeDtypeStruct((56, 128), bf16),
    )
    gathered, *rest = pl.pallas_call(
        gather_kernel,
        out_shape=(jax.ShapeDtypeStruct((7168, 1152), bf16), *small),
        in_specs=[pl.BlockSpec(memory_space=HBM)] * 9,
        out_specs=(pl.BlockSpec(memory_space=VMEM),) * 5,
        scratch_shapes=[
            pltpu.VMEM((448, 1152), f32),
            pltpu.VMEM((448, 1152), f32),
            pltpu.VMEM((1, 448), f32),
            pltpu.VMEM((2, 1, 56), f32),
            pltpu.VMEM((1, 512), f32),
            pltpu.VMEM((512, 128), f32),
            pltpu.VMEM((16, 7, 1, 128), f32),
            pltpu.VMEM((16, 2, 1, 128), f32),
            pltpu.VMEM((9, 1, 128), f32),
            pltpu.VMEM((8, 128), f32),
            pltpu.VMEM((8, 16, 1, 128), f32),
            pltpu.VMEM((56, 128), f32),
            pltpu.VMEM((3, EARLY, 1152), f32),
            dma((BLOCK // PIECE + 1,)),
            dma((2,)),
            pltpu.SemaphoreType.REGULAR,
            dma((2,)),
            dma((2,)),
            dma((2,)),
            dma((2,)),
            dma((2,)),
            dma((3, AHEAD)),
            dma((3, SLOTS)),
            dma,
            dma,
            dma((2,)),
            dma((2,)),
        ],
        compiler_params=pltpu.CompilerParams(
            collective_id=0, has_side_effects=True, vmem_limit_bytes=32 << 20
        ),
    )(*inputs)
    query, key, value, *outs = pl.pallas_call(
        write_kernel,
        out_shape=(
            jax.ShapeDtypeStruct((7168, 896), bf16),
            jax.ShapeDtypeStruct((7168, 128), bf16),
            jax.ShapeDtypeStruct((7168, 128), bf16),
            *small,
        ),
        in_specs=[pl.BlockSpec(memory_space=VMEM)] * 5,
        out_specs=(pl.BlockSpec(memory_space=HBM),) * 7,
        scratch_shapes=[dma((7,))],
        compiler_params=pltpu.CompilerParams(vmem_limit_bytes=20 << 20),
    )(gathered, *rest)
    return (query, key, value, *(x.reshape(-1) for x in outs))


def solution(mesh):
    in_specs = (
        P("rows", "width"),
        P("rows", "width"),
        P("rows", "width"),
        P("rows", "width"),
        P("rows", "width"),
        P("rows", "width"),
        P("rows"),
        P(("rows", "width")),
        P(("rows", "width")),
    )
    out_specs = (
        P(None, "width"),
        P(None, "width"),
        P(None, "width"),
        P("width"),
        P("width"),
        P("width"),
        P(),
    )
    return jax.shard_map(shards, mesh=mesh, in_specs=in_specs, out_specs=out_specs, check_vma=False)
```

```python
import functools

import jax
import jax.numpy as jnp
from jax import lax
from jax.experimental import pallas as pl
from jax.experimental.pallas import tpu as pltpu
from jax.sharding import PartitionSpec as P

MESH = pl.DeviceIdType.MESH
HBM = pltpu.MemorySpace.HBM
VMEM = pltpu.MemorySpace.VMEM

BLOCK = 448
HALF = 224
PIECE = 112
QUERY = (0, 896)
KEYVALUE = (896, 256)
ALL = (0, 1152)
EARLY = 32
LAST = 8
LOW = ((EARLY, 96), (96, 160), (160, 224))
HIGH = ((224, 304), (304, 368), (368, 448))


def own(*parts):
    return [(0, 0, rows, columns) for rows, columns in parts]


def relay(dy, dz, *rows):
    return [(dy, dz, r, ALL) for r in rows]


UP = (
    own(((EARLY, 160), KEYVALUE), (LOW[0], QUERY), (LOW[1], QUERY), (LOW[2], ALL), *((r, ALL) for r in HIGH))
    + relay(-1, 0, (0, 96), *LOW[1:])
    + relay(0, 1, (224, 304), (304, 376))
    + relay(-1, 1, (0, 96), (96, 160), (160, 200), (200, 216), (216, 224))
)
DOWN = (
    own(((224, 368), KEYVALUE), (HIGH[0], QUERY), (HIGH[1], QUERY), (HIGH[2], ALL), *((r, ALL) for r in LOW))
    + relay(1, 0, *HIGH)
    + relay(0, 1, (0, 80), (80, 152))
    + relay(1, 1, (224, 304), (304, 368), (368, 424), (424, 440), (440, 448))
)
ACROSS = (
    own(
        ((EARLY, 160), KEYVALUE),
        (LOW[0], QUERY),
        (HIGH[0], ALL),
        (LOW[1], QUERY),
        (HIGH[1], ALL),
        (LOW[2], ALL),
        (HIGH[2], ALL),
    )
    + relay(-1, 0, (0, 96))
    + relay(1, 0, HIGH[0])
    + relay(-1, 0, LOW[1])
    + relay(1, 0, HIGH[1])
    + relay(-1, 0, LOW[2])
    + relay(1, 0, HIGH[2])
    + relay(-1, 0, (376, 448))
    + relay(1, 0, (152, 200), (200, 216), (216, 224))
)
SENT = (UP, DOWN, ACROSS)
SHIFT = ((1, 0), (-1, 0), (0, 1))
STEPS = len(UP)
AHEAD = 2
SLOTS = 2 * AHEAD + 2
GATE = 1
GAIN_STEPS = (5, 8, 9, 12)
FARTHEST = ((2, 1), (1, 1), (3, 1), (2, 0), (1, 0), (3, 0), (0, 1), (0, 0))


def arriving(link, step):
    dy, dz, rows, columns = SENT[link][step]
    sy, sz = SHIFT[link]
    return ((dy - sy) % 4, (dz - sz) % 2, rows, columns)


ARRIVALS = [(l, s) for s in range(STEPS) for l in range(3)]


def needed(item):
    dy, dz, rows, _ = item
    for l, s in ARRIVALS:
        ay, az, have, _ = arriving(l, s)
        if (ay, az) == (dy % 4, dz % 2) and have[0] < rows[1] and rows[0] < have[1]:
            yield l, s


def gather_kernel(
    one_query,
    other_query,
    one_key,
    other_key,
    one_value,
    other_value,
    share_input,
    train_input,
    step_input,
    gathered,
    scale_query,
    scale_key,
    scale_value,
    gain,
    first,
    second,
    share,
    gains,
    share_row,
    share_tile,
    sums_late,
    sums_early,
    inverse,
    gain_tile,
    gain_rows,
    gain_flat,
    early_rows,
    load_sem,
    small_sem,
    entered,
    sum_send,
    sum_recv,
    row_sem,
    gate_sem,
    gain_sem,
    link_send,
    link_recv,
    core_send,
    core_recv,
    early_sem,
    last_sem,
):
    me = lax.axis_index("rows")
    column = lax.axis_index("width")
    core = lax.rem(me, 2)
    y = lax.rem(me // 2, 4)
    z = me // 8

    def device(dy, dz, on):
        return lax.rem(z + dz + 2, 2) * 8 + lax.rem(y + dy + 4, 4) * 2 + on

    at_gate = me == GATE
    barrier = pltpu.get_barrier_semaphore()
    others = [(dy, dz, on) for dy, dz in FARTHEST for on in (0, 1) if (dy, dz, on) != (0, 0, 0)]
    def signal(peers):
        for dy, dz, on in peers:
            peer = device(dy, dz, lax.rem(core + on, 2))

            @pl.when(peer != GATE)
            def _():
                pl.semaphore_signal(barrier, inc=1, device_id=(peer, column), device_id_type=MESH)

    signal(others[:6])

    small = [
        pltpu.make_async_copy(share_input, share, small_sem.at[0]),
        pltpu.make_async_copy(train_input, gains.at[0], small_sem.at[1]),
        pltpu.make_async_copy(step_input, gains.at[1], small_sem.at[1]),
    ]
    pieces = BLOCK // PIECE
    small[0].start()
    for source, target, at in (
        (one_key, first, 896),
        (other_key, second, 896),
        (one_value, first, 1024),
        (other_value, second, 1024),
    ):
        pltpu.make_async_copy(source, target.at[:, pl.ds(at, 128)], load_sem.at[pieces]).start()
    for piece in range(pieces):
        rows = pl.ds(piece * PIECE, PIECE)
        for source, target in ((one_query, first), (other_query, second)):
            pltpu.make_async_copy(source.at[rows, :], target.at[rows, pl.ds(0, 896)], load_sem.at[piece]).start()
    for copy in small[1:]:
        copy.start()

    signal(others[6:])

    @pl.when(at_gate)
    def _():
        for k in range(1, 8):
            pl.semaphore_signal(barrier, inc=1, device_id=(me, lax.rem(column + k, 8)), device_id_type=MESH)

    def loaded(number, rows, columns):
        place = (pl.ds(0, rows), pl.ds(0, columns))
        pltpu.make_async_copy(first.at[place], second.at[place], load_sem.at[number]).wait()

    small[0].wait()
    share_row[...] = jnp.zeros_like(share_row)
    share_row[:, 0:BLOCK] = share[...]
    for part in range(4):
        lanes = share_row[:, part * 128 : (part + 1) * 128]
        share_tile[pl.ds(part * 128, 128), :] = jnp.transpose(jnp.broadcast_to(lanes, (128, 128)))

    def mix(start, rows, tiles, total):
        def body(i, total):
            total = list(total)
            for part in range(2):
                at = pl.ds(pl.multiple_of(start + i * 16 + part * 8, 8), 8)
                mine = share_tile[at, :]
                rest = 1.0 - mine
                for n, j in enumerate(tiles):
                    lanes = slice(j * 128, (j + 1) * 128)
                    result = mine * first[at, lanes] + rest * second[at, lanes]
                    first[at, lanes] = result
                    total[n] = total[n] + result * result
            return tuple(total)

        return lax.fori_loop(0, rows // 16, body, total, unroll=2 if len(tiles) == 2 else 1)

    def zeros(n):
        return tuple(jnp.zeros((8, 128), jnp.float32) for _ in range(n))

    def send_sum(sums, n, dy, dz, on):
        return pltpu.make_async_remote_copy(
            src_ref=sums.at[me],
            dst_ref=sums.at[me],
            send_sem=sum_send.at[n],
            recv_sem=sum_recv.at[n],
            device_id=(device(dy, dz, lax.rem(core + on, 2)), column),
            device_id_type=MESH,
        )

    def all_sums(sums, n):
        return pltpu.make_async_remote_copy(
            src_ref=sums.at[pl.ds(0, 15)],
            dst_ref=sums.at[pl.ds(0, 15)],
            send_sem=sum_send.at[n],
            recv_sem=sum_recv.at[n],
            device_id=(device(0, 0, 1 - core), column),
            device_id_type=MESH,
        )

    def grand(sums, tiles):
        total = [sums[0, n] for n in range(len(tiles))]
        for other in range(1, 16):
            total = [t + sums[other, n] for n, t in enumerate(total)]
        for j, t in zip(tiles, total):
            scale = jnp.sqrt(t)
            if j < 7:
                scale_query[j : j + 1, :] = scale
            elif j == 7:
                scale_key[...] = scale
            else:
                scale_value[...] = scale
            inverse[j] = 1.0 / scale

    late, early = tuple(range(7)), (7, 8)

    loaded(pieces, BLOCK, 512)
    for n, t in enumerate(mix(0, BLOCK, early, zeros(2))):
        sums_early[me, n] = jnp.sum(t, axis=0, keepdims=True)

    @pl.when(jnp.logical_not(at_gate))
    def _():
        pl.semaphore_wait(barrier, 15)

    @pl.when(me == GATE - 1)
    def _():
        pl.semaphore_signal(entered, inc=1, device_id=(GATE, column), device_id_type=MESH)

    @pl.when(at_gate)
    def _():
        pl.semaphore_wait(entered, 1)

    for to in others:
        send_sum(sums_early, 0, *to).start()
    total = zeros(7)
    for piece in range(pieces):
        loaded(piece, 2 * PIECE, 896)
        total = mix(piece * PIECE, PIECE, late, total)
    for n, t in enumerate(total):
        sums_late[me, n] = jnp.sum(t, axis=0, keepdims=True)
    for to in others:
        send_sum(sums_late, 1, *to).start()

    def early_copy(link):
        sy, sz = SHIFT[link]
        return pltpu.make_async_remote_copy(
            src_ref=first.at[pl.ds(0, EARLY), :],
            dst_ref=early_rows.at[link],
            send_sem=early_sem.at[0],
            recv_sem=early_sem.at[1],
            device_id=(device(sy, sz, core), column),
            device_id_type=MESH,
        )

    def all_early():
        return pltpu.make_async_remote_copy(
            src_ref=early_rows,
            dst_ref=early_rows,
            send_sem=early_sem.at[0],
            recv_sem=early_sem.at[1],
            device_id=(device(0, 0, 1 - core), column),
            device_id_type=MESH,
        )

    for link in range(3):
        early_copy(link).start()

    pltpu.make_async_copy(gains, gains, small_sem.at[1]).wait()
    gain_tile[...] = jnp.zeros_like(gain_tile)
    gain_tile[0:1, 0:56] = (gains[0] + gains[1]).astype(jnp.bfloat16).astype(jnp.float32)
    place = lax.rem(56 * (lax.rem(me, 2) * 8 + column), 128)
    gain_rows[column, me] = pltpu.roll(gain_tile[...], place, 1)[0:1, :]

    def send_row():
        return pltpu.make_async_remote_copy(
            src_ref=gain_rows.at[column, me],
            dst_ref=gain_rows.at[column, me],
            send_sem=row_sem.at[0],
            recv_sem=row_sem.at[1],
            device_id=(GATE, column),
            device_id_type=MESH,
        )

    def all_rows():
        return pltpu.make_async_remote_copy(
            src_ref=gain_rows.at[column, pl.ds(0, 15)],
            dst_ref=gain_rows.at[column, pl.ds(0, 15)],
            send_sem=row_sem.at[0],
            recv_sem=row_sem.at[1],
            device_id=(GATE - 1, column),
            device_id_type=MESH,
        )

    def send_group(k):
        return pltpu.make_async_remote_copy(
            src_ref=gain_rows.at[column],
            dst_ref=gain_rows.at[column],
            send_sem=gate_sem.at[0],
            recv_sem=gate_sem.at[1],
            device_id=(GATE, lax.rem(column + k, 8)),
            device_id_type=MESH,
        )

    def all_groups():
        return pltpu.make_async_remote_copy(
            src_ref=gain_rows.at[pl.ds(0, 7)],
            dst_ref=gain_rows.at[pl.ds(0, 7)],
            send_sem=gate_sem.at[0],
            recv_sem=gate_sem.at[1],
            device_id=(GATE - 1, column),
            device_id_type=MESH,
        )

    def send_gain(to):
        return pltpu.make_async_remote_copy(
            src_ref=gain,
            dst_ref=gain,
            send_sem=gain_sem.at[0],
            recv_sem=gain_sem.at[1],
            device_id=(to, column),
            device_id_type=MESH,
        )

    def compose():
        lane = lax.broadcasted_iota(jnp.int32, (1, 128), 1)
        for group in range(8):
            rows = [jnp.zeros((1, 128), jnp.float32) for _ in range(8)]
            for j in range(16):
                values = gain_rows[j % 8, group * 2 + j // 8]
                row, at = (56 * j) // 128, (56 * j) % 128
                rows[row] = jnp.where((lane >= at) & (lane < at + 56), values, rows[row])
                if at + 56 > 128:
                    rows[row + 1] = jnp.where(lane < at + 56 - 128, values, rows[row + 1])
            for row in range(7):
                gain_flat[group * 7 + row : group * 7 + row + 1, :] = rows[row]
        gain[...] = gain_flat[...].astype(jnp.bfloat16)

    spread = [to for to in range(16) if to % 2 == GATE % 2 and to != GATE] + [GATE - 1]

    def place_of(item, on):
        dy, dz, (low, high), (left, width) = item
        start = pl.multiple_of(device(dy, dz, on) * BLOCK + low, 8)
        return (pl.ds(start, high - low), pl.ds(left, width))

    def link_copy(link, step, item):
        place = place_of(item, core)
        sy, sz = SHIFT[link]
        return pltpu.make_async_remote_copy(
            src_ref=gathered.at[place],
            dst_ref=gathered.at[place],
            send_sem=link_send.at[link, step % AHEAD],
            recv_sem=link_recv.at[link, step % SLOTS],
            device_id=(device(sy, sz, core), column),
            device_id_type=MESH,
        )

    def last_copy(link):
        place = place_of(SENT[link][STEPS - 1], core)
        sy, sz = SHIFT[link]
        return pltpu.make_async_remote_copy(
            src_ref=gathered.at[place],
            dst_ref=gathered.at[place],
            send_sem=last_sem.at[0],
            recv_sem=last_sem.at[1],
            device_id=(device(sy, sz, 1 - core), column),
            device_id_type=MESH,
        )

    def core_copy(place):
        return pltpu.make_async_remote_copy(
            src_ref=gathered.at[place],
            dst_ref=gathered.at[place],
            send_sem=core_send,
            recv_sem=core_recv,
            device_id=(device(0, 0, 1 - core), column),
            device_id_type=MESH,
        )

    def normalise(tiles):
        def body(i, _):
            at = pl.multiple_of(i * 16, 16)
            to = pl.multiple_of(me * BLOCK + i * 16, 16)
            for j in tiles:
                lanes = slice(j * 128, (j + 1) * 128)
                gathered[pl.ds(to, 16), lanes] = (first[pl.ds(at, 16), lanes] * inverse[j]).astype(jnp.bfloat16)
            return 0

        lax.fori_loop(0, BLOCK // 16, body, 0)

    def normalise_early():
        for link, (sy, sz) in enumerate(SHIFT):
            for i in range(EARLY // 16):
                to = pl.multiple_of(device(-sy, -sz, core) * BLOCK + i * 16, 16)
                for j in range(9):
                    lanes = slice(j * 128, (j + 1) * 128)
                    values = early_rows[link, i * 16 : (i + 1) * 16, lanes] * inverse[j]
                    gathered[pl.ds(to, 16), lanes] = values.astype(jnp.bfloat16)

    arrived = set()

    def receive(link, step):
        if (link, step) in arrived:
            return
        arrived.add((link, step))
        item = arriving(link, step)
        link_copy(link, step, item).wait_recv()
        if step < STEPS - 1:
            core_copy(place_of(item, core)).start()

    all_sums(sums_early, 0).wait_recv()
    grand(sums_early, early)
    normalise(early)

    for step in range(STEPS):
        for link in range(3):
            if step >= AHEAD:
                link_copy(link, step - AHEAD, SENT[link][step - AHEAD]).wait_send()
            item = SENT[link][step]
            if item[:2] != (0, 0):
                for arrival in needed(item):
                    receive(*arrival)
            link_copy(link, step, item).start()
            if step == STEPS - 1:
                last_copy(link).start()
        if step == 0:

            @pl.when(jnp.logical_not(at_gate))
            def _():
                send_row().start()

            all_sums(sums_late, 1).wait_recv()
            grand(sums_late, late)
            normalise(late)
        if step == 1:
            all_early().wait_recv()
            normalise_early()
        if step == 3:
            for sy, sz in SHIFT:
                core_copy(place_of((-sy, -sz, (0, EARLY), ALL), core)).start()
        if step in (1, 2):
            core_copy(place_of((0, 0, ((step - 1) * HALF, step * HALF), ALL), core)).start()
        if step == GAIN_STEPS[0]:

            @pl.when(at_gate)
            def _():
                all_rows().wait_recv()
                pl.semaphore_wait(barrier, 7)
                for k in range(1, 8):
                    send_group(k).start()

        if step == GAIN_STEPS[1]:

            @pl.when(at_gate)
            def _():
                all_groups().wait_recv()
                compose()

        if step == GAIN_STEPS[2]:

            @pl.when(at_gate)
            def _():
                for to in spread:
                    send_gain(to).start()

        if step == GAIN_STEPS[3]:

            @pl.when(jnp.logical_and(jnp.logical_not(at_gate), core == GATE % 2))
            def _():
                send_gain(me).wait_recv()
                send_gain(device(0, 0, 1 - core)).start()

        if step >= AHEAD:
            for link in range(3):
                receive(link, step - AHEAD)

    for step in range(STEPS - AHEAD, STEPS):
        for link in range(3):
            receive(link, step)
    for step in range(STEPS - AHEAD, STEPS):
        for link in range(3):
            link_copy(link, step, SENT[link][step]).wait_send()
    all_early().wait_send()
    all_sums(sums_early, 0).wait_send()
    all_sums(sums_late, 1).wait_send()

    @pl.when(core != GATE % 2)
    def _():
        send_gain(me).wait_recv()

    @pl.when(at_gate)
    def _():
        all_groups().wait_send()
        gains_sent = gathered.at[pl.ds(0, 448), pl.ds(0, 128)]
        pltpu.make_async_copy(gains_sent, gains_sent, gain_sem.at[0]).wait()

    @pl.when(jnp.logical_not(at_gate))
    def _():
        send_row().wait_send()

        @pl.when(core == GATE % 2)
        def _():
            send_gain(me).wait_send()

    half = core_copy((pl.ds(0, 8 * BLOCK - 3 * LAST), pl.ds(0, 1152)))
    half.wait_send()
    half.wait_recv()
    rows = gathered.at[pl.ds(0, 3 * LAST), :]
    for n in range(2):
        pltpu.make_async_copy(rows, rows, last_sem.at[n]).wait()


def write_kernel(gathered, *rest):
    small, (query, key, value), outs, sem = rest[:4], rest[4:7], rest[7:11], rest[11]
    parts = 4
    rows = gathered.shape[0] // parts
    for part in range(parts):
        at = pl.ds(part * rows, rows)
        pltpu.make_async_copy(gathered.at[at, pl.ds(0, 896)], query.at[at, :], sem.at[0]).start()
    others = [
        pltpu.make_async_copy(gathered.at[:, pl.ds(896, 128)], key, sem.at[1]),
        pltpu.make_async_copy(gathered.at[:, pl.ds(1024, 128)], value, sem.at[2]),
    ]
    for source, target in zip(small, outs):
        others.append(pltpu.make_async_copy(source, target, sem.at[len(others) + 1]))
    for copy in others:
        copy.start()
    pltpu.make_async_copy(gathered.at[:, pl.ds(0, 896)], query, sem.at[0]).wait()
    for copy in others:
        copy.wait()


def shards(
    one_query,
    other_query,
    one_key,
    other_key,
    one_value,
    other_value,
    mix_share,
    norm_train,
    norm_step,
):
    dma = pltpu.SemaphoreType.DMA
    f32, bf16 = jnp.float32, jnp.bfloat16
    inputs = [
        pltpu.with_memory_space_constraint(x, HBM)
        for x in (
            one_query,
            other_query,
            one_key,
            other_key,
            one_value,
            other_value,
            mix_share.reshape(1, 448),
            norm_train.reshape(1, 56),
            norm_step.reshape(1, 56),
        )
    ]
    small = (
        jax.ShapeDtypeStruct((7, 128), f32),
        jax.ShapeDtypeStruct((1, 128), f32),
        jax.ShapeDtypeStruct((1, 128), f32),
        jax.ShapeDtypeStruct((56, 128), bf16),
    )
    gathered, *rest = pl.pallas_call(
        gather_kernel,
        out_shape=(jax.ShapeDtypeStruct((7168, 1152), bf16), *small),
        in_specs=[pl.BlockSpec(memory_space=HBM)] * 9,
        out_specs=(pl.BlockSpec(memory_space=VMEM),) * 5,
        scratch_shapes=[
            pltpu.VMEM((448, 1152), f32),
            pltpu.VMEM((448, 1152), f32),
            pltpu.VMEM((1, 448), f32),
            pltpu.VMEM((2, 1, 56), f32),
            pltpu.VMEM((1, 512), f32),
            pltpu.VMEM((512, 128), f32),
            pltpu.VMEM((16, 7, 1, 128), f32),
            pltpu.VMEM((16, 2, 1, 128), f32),
            pltpu.VMEM((9, 1, 128), f32),
            pltpu.VMEM((8, 128), f32),
            pltpu.VMEM((8, 16, 1, 128), f32),
            pltpu.VMEM((56, 128), f32),
            pltpu.VMEM((3, EARLY, 1152), f32),
            dma((BLOCK // PIECE + 1,)),
            dma((2,)),
            pltpu.SemaphoreType.REGULAR,
            dma((2,)),
            dma((2,)),
            dma((2,)),
            dma((2,)),
            dma((2,)),
            dma((3, AHEAD)),
            dma((3, SLOTS)),
            dma,
            dma,
            dma((2,)),
            dma((2,)),
        ],
        compiler_params=pltpu.CompilerParams(
            collective_id=0, has_side_effects=True, vmem_limit_bytes=32 << 20
        ),
    )(*inputs)
    query, key, value, *outs = pl.pallas_call(
        write_kernel,
        out_shape=(
            jax.ShapeDtypeStruct((7168, 896), bf16),
            jax.ShapeDtypeStruct((7168, 128), bf16),
            jax.ShapeDtypeStruct((7168, 128), bf16),
            *small,
        ),
        in_specs=[pl.BlockSpec(memory_space=VMEM)] * 5,
        out_specs=(pl.BlockSpec(memory_space=HBM),) * 7,
        scratch_shapes=[dma((7,))],
        compiler_params=pltpu.CompilerParams(vmem_limit_bytes=20 << 20),
    )(gathered, *rest)
    return (query, key, value, *(x.reshape(-1) for x in outs))


def solution(mesh):
    in_specs = (
        P("rows", "width"),
        P("rows", "width"),
        P("rows", "width"),
        P("rows", "width"),
        P("rows", "width"),
        P("rows", "width"),
        P("rows"),
        P(("rows", "width")),
        P(("rows", "width")),
    )
    out_specs = (
        P(None, "width"),
        P(None, "width"),
        P(None, "width"),
        P("width"),
        P("width"),
        P("width"),
        P(),
    )
    return jax.shard_map(shards, mesh=mesh, in_specs=in_specs, out_specs=out_specs, check_vma=False)
```

```python
import functools

import jax
import jax.numpy as jnp
from jax import lax
from jax.experimental import pallas as pl
from jax.experimental.pallas import tpu as pltpu
from jax.sharding import PartitionSpec as P

MESH = pl.DeviceIdType.MESH
HBM = pltpu.MemorySpace.HBM
VMEM = pltpu.MemorySpace.VMEM

BLOCK = 448
HALF = 224
PIECE = 112
QUERY = (0, 896)
KEYVALUE = (896, 256)
ALL = (0, 1152)
EARLY = 32
LAST = 8
LOW = ((EARLY, 96), (96, 160), (160, 224))
HIGH = ((224, 304), (304, 368), (368, 448))


def own(*parts):
    return [(0, 0, rows, columns) for rows, columns in parts]


def relay(dy, dz, *rows):
    return [(dy, dz, r, ALL) for r in rows]


UP = (
    own(((EARLY, 224), KEYVALUE), (LOW[0], QUERY), (LOW[1], QUERY), (LOW[2], QUERY), *((r, ALL) for r in HIGH))
    + relay(-1, 0, (0, 96), *LOW[1:])
    + relay(0, 1, (224, 304), (304, 376))
    + relay(-1, 1, (0, 96), (96, 160), (160, 200), (200, 216), (216, 224))
)
DOWN = (
    own(((224, 448), KEYVALUE), (HIGH[0], QUERY), (HIGH[1], QUERY), (HIGH[2], QUERY), *((r, ALL) for r in LOW))
    + relay(1, 0, *HIGH)
    + relay(0, 1, (0, 80), (80, 152))
    + relay(1, 1, (224, 304), (304, 368), (368, 424), (424, 440), (440, 448))
)
ACROSS = (
    own(
        ((EARLY, 224), KEYVALUE),
        (LOW[0], QUERY),
        (HIGH[0], ALL),
        (LOW[1], QUERY),
        (HIGH[1], ALL),
        (LOW[2], QUERY),
        (HIGH[2], ALL),
    )
    + relay(-1, 0, (0, 96))
    + relay(1, 0, HIGH[0])
    + relay(-1, 0, LOW[1])
    + relay(1, 0, HIGH[1])
    + relay(-1, 0, LOW[2])
    + relay(1, 0, HIGH[2])
    + relay(-1, 0, (376, 448))
    + relay(1, 0, (152, 200), (200, 216), (216, 224))
)
SENT = (UP, DOWN, ACROSS)
SHIFT = ((1, 0), (-1, 0), (0, 1))
STEPS = len(UP)
AHEAD = 2
SLOTS = 2 * AHEAD + 2
GATE = 1
GAIN_STEPS = (5, 8, 9, 12)
FARTHEST = ((2, 1), (1, 1), (3, 1), (2, 0), (1, 0), (3, 0), (0, 1), (0, 0))


def arriving(link, step):
    dy, dz, rows, columns = SENT[link][step]
    sy, sz = SHIFT[link]
    return ((dy - sy) % 4, (dz - sz) % 2, rows, columns)


ARRIVALS = [(l, s) for s in range(STEPS) for l in range(3)]


def needed(item):
    dy, dz, rows, _ = item
    for l, s in ARRIVALS:
        ay, az, have, _ = arriving(l, s)
        if (ay, az) == (dy % 4, dz % 2) and have[0] < rows[1] and rows[0] < have[1]:
            yield l, s


def gather_kernel(
    one_query,
    other_query,
    one_key,
    other_key,
    one_value,
    other_value,
    share_input,
    train_input,
    step_input,
    gathered,
    scale_query,
    scale_key,
    scale_value,
    gain,
    first,
    second,
    share,
    gains,
    share_row,
    share_tile,
    sums_late,
    sums_early,
    inverse,
    gain_tile,
    gain_rows,
    gain_flat,
    early_rows,
    load_sem,
    small_sem,
    entered,
    sum_send,
    sum_recv,
    row_sem,
    gate_sem,
    gain_sem,
    link_send,
    link_recv,
    core_send,
    core_recv,
    early_sem,
    last_sem,
):
    me = lax.axis_index("rows")
    column = lax.axis_index("width")
    core = lax.rem(me, 2)
    y = lax.rem(me // 2, 4)
    z = me // 8

    def device(dy, dz, on):
        return lax.rem(z + dz + 2, 2) * 8 + lax.rem(y + dy + 4, 4) * 2 + on

    at_gate = me == GATE
    barrier = pltpu.get_barrier_semaphore()
    others = [(dy, dz, on) for dy, dz in FARTHEST for on in (0, 1) if (dy, dz, on) != (0, 0, 0)]
    def signal(peers):
        for dy, dz, on in peers:
            peer = device(dy, dz, lax.rem(core + on, 2))

            @pl.when(peer != GATE)
            def _():
                pl.semaphore_signal(barrier, inc=1, device_id=(peer, column), device_id_type=MESH)

    signal(others[:6])

    small = [
        pltpu.make_async_copy(share_input, share, small_sem.at[0]),
        pltpu.make_async_copy(train_input, gains.at[0], small_sem.at[1]),
        pltpu.make_async_copy(step_input, gains.at[1], small_sem.at[1]),
    ]
    pieces = BLOCK // PIECE
    small[0].start()
    for source, target, at in (
        (one_key, first, 896),
        (other_key, second, 896),
        (one_value, first, 1024),
        (other_value, second, 1024),
    ):
        pltpu.make_async_copy(source, target.at[:, pl.ds(at, 128)], load_sem.at[pieces]).start()
    for piece in range(pieces):
        rows = pl.ds(piece * PIECE, PIECE)
        for source, target in ((one_query, first), (other_query, second)):
            pltpu.make_async_copy(source.at[rows, :], target.at[rows, pl.ds(0, 896)], load_sem.at[piece]).start()
    for copy in small[1:]:
        copy.start()

    signal(others[6:])

    @pl.when(at_gate)
    def _():
        for k in range(1, 8):
            pl.semaphore_signal(barrier, inc=1, device_id=(me, lax.rem(column + k, 8)), device_id_type=MESH)

    def loaded(number, rows, columns):
        place = (pl.ds(0, rows), pl.ds(0, columns))
        pltpu.make_async_copy(first.at[place], second.at[place], load_sem.at[number]).wait()

    small[0].wait()
    share_row[...] = jnp.zeros_like(share_row)
    share_row[:, 0:BLOCK] = share[...]
    for part in range(4):
        lanes = share_row[:, part * 128 : (part + 1) * 128]
        share_tile[pl.ds(part * 128, 128), :] = jnp.transpose(jnp.broadcast_to(lanes, (128, 128)))

    def mix(start, rows, tiles, total):
        def body(i, total):
            total = list(total)
            for part in range(2):
                at = pl.ds(pl.multiple_of(start + i * 16 + part * 8, 8), 8)
                mine = share_tile[at, :]
                rest = 1.0 - mine
                for n, j in enumerate(tiles):
                    lanes = slice(j * 128, (j + 1) * 128)
                    result = mine * first[at, lanes] + rest * second[at, lanes]
                    first[at, lanes] = result
                    total[n] = total[n] + result * result
            return tuple(total)

        return lax.fori_loop(0, rows // 16, body, total, unroll=2 if len(tiles) == 2 else 1)

    def zeros(n):
        return tuple(jnp.zeros((8, 128), jnp.float32) for _ in range(n))

    def send_sum(sums, n, dy, dz, on):
        return pltpu.make_async_remote_copy(
            src_ref=sums.at[me],
            dst_ref=sums.at[me],
            send_sem=sum_send.at[n],
            recv_sem=sum_recv.at[n],
            device_id=(device(dy, dz, lax.rem(core + on, 2)), column),
            device_id_type=MESH,
        )

    def all_sums(sums, n):
        return pltpu.make_async_remote_copy(
            src_ref=sums.at[pl.ds(0, 15)],
            dst_ref=sums.at[pl.ds(0, 15)],
            send_sem=sum_send.at[n],
            recv_sem=sum_recv.at[n],
            device_id=(device(0, 0, 1 - core), column),
            device_id_type=MESH,
        )

    def grand(sums, tiles):
        total = [sums[0, n] for n in range(len(tiles))]
        for other in range(1, 16):
            total = [t + sums[other, n] for n, t in enumerate(total)]
        for j, t in zip(tiles, total):
            scale = jnp.sqrt(t)
            if j < 7:
                scale_query[j : j + 1, :] = scale
            elif j == 7:
                scale_key[...] = scale
            else:
                scale_value[...] = scale
            inverse[j] = 1.0 / scale

    late, early = tuple(range(7)), (7, 8)

    loaded(pieces, BLOCK, 512)
    for n, t in enumerate(mix(0, BLOCK, early, zeros(2))):
        sums_early[me, n] = jnp.sum(t, axis=0, keepdims=True)

    @pl.when(jnp.logical_not(at_gate))
    def _():
        pl.semaphore_wait(barrier, 15)

    @pl.when(me == GATE - 1)
    def _():
        pl.semaphore_signal(entered, inc=1, device_id=(GATE, column), device_id_type=MESH)

    @pl.when(at_gate)
    def _():
        pl.semaphore_wait(entered, 1)

    for to in others:
        send_sum(sums_early, 0, *to).start()
    total = zeros(7)
    for piece in range(pieces):
        loaded(piece, 2 * PIECE, 896)
        total = mix(piece * PIECE, PIECE, late, total)
    for n, t in enumerate(total):
        sums_late[me, n] = jnp.sum(t, axis=0, keepdims=True)
    for to in others:
        send_sum(sums_late, 1, *to).start()

    def early_copy(link):
        sy, sz = SHIFT[link]
        return pltpu.make_async_remote_copy(
            src_ref=first.at[pl.ds(0, EARLY), :],
            dst_ref=early_rows.at[link],
            send_sem=early_sem.at[0],
            recv_sem=early_sem.at[1],
            device_id=(device(sy, sz, core), column),
            device_id_type=MESH,
        )

    def all_early():
        return pltpu.make_async_remote_copy(
            src_ref=early_rows,
            dst_ref=early_rows,
            send_sem=early_sem.at[0],
            recv_sem=early_sem.at[1],
            device_id=(device(0, 0, 1 - core), column),
            device_id_type=MESH,
        )

    for link in range(3):
        early_copy(link).start()

    pltpu.make_async_copy(gains, gains, small_sem.at[1]).wait()
    gain_tile[...] = jnp.zeros_like(gain_tile)
    gain_tile[0:1, 0:56] = (gains[0] + gains[1]).astype(jnp.bfloat16).astype(jnp.float32)
    place = lax.rem(56 * (lax.rem(me, 2) * 8 + column), 128)
    gain_rows[column, me] = pltpu.roll(gain_tile[...], place, 1)[0:1, :]

    def send_row():
        return pltpu.make_async_remote_copy(
            src_ref=gain_rows.at[column, me],
            dst_ref=gain_rows.at[column, me],
            send_sem=row_sem.at[0],
            recv_sem=row_sem.at[1],
            device_id=(GATE, column),
            device_id_type=MESH,
        )

    def all_rows():
        return pltpu.make_async_remote_copy(
            src_ref=gain_rows.at[column, pl.ds(0, 15)],
            dst_ref=gain_rows.at[column, pl.ds(0, 15)],
            send_sem=row_sem.at[0],
            recv_sem=row_sem.at[1],
            device_id=(GATE - 1, column),
            device_id_type=MESH,
        )

    def send_group(k):
        return pltpu.make_async_remote_copy(
            src_ref=gain_rows.at[column],
            dst_ref=gain_rows.at[column],
            send_sem=gate_sem.at[0],
            recv_sem=gate_sem.at[1],
            device_id=(GATE, lax.rem(column + k, 8)),
            device_id_type=MESH,
        )

    def all_groups():
        return pltpu.make_async_remote_copy(
            src_ref=gain_rows.at[pl.ds(0, 7)],
            dst_ref=gain_rows.at[pl.ds(0, 7)],
            send_sem=gate_sem.at[0],
            recv_sem=gate_sem.at[1],
            device_id=(GATE - 1, column),
            device_id_type=MESH,
        )

    def send_gain(to):
        return pltpu.make_async_remote_copy(
            src_ref=gain,
            dst_ref=gain,
            send_sem=gain_sem.at[0],
            recv_sem=gain_sem.at[1],
            device_id=(to, column),
            device_id_type=MESH,
        )

    def compose():
        lane = lax.broadcasted_iota(jnp.int32, (1, 128), 1)
        for group in range(8):
            rows = [jnp.zeros((1, 128), jnp.float32) for _ in range(8)]
            for j in range(16):
                values = gain_rows[j % 8, group * 2 + j // 8]
                row, at = (56 * j) // 128, (56 * j) % 128
                rows[row] = jnp.where((lane >= at) & (lane < at + 56), values, rows[row])
                if at + 56 > 128:
                    rows[row + 1] = jnp.where(lane < at + 56 - 128, values, rows[row + 1])
            for row in range(7):
                gain_flat[group * 7 + row : group * 7 + row + 1, :] = rows[row]
        gain[...] = gain_flat[...].astype(jnp.bfloat16)

    spread = [to for to in range(16) if to % 2 == GATE % 2 and to != GATE] + [GATE - 1]

    def place_of(item, on):
        dy, dz, (low, high), (left, width) = item
        start = pl.multiple_of(device(dy, dz, on) * BLOCK + low, 8)
        return (pl.ds(start, high - low), pl.ds(left, width))

    def link_copy(link, step, item):
        place = place_of(item, core)
        sy, sz = SHIFT[link]
        return pltpu.make_async_remote_copy(
            src_ref=gathered.at[place],
            dst_ref=gathered.at[place],
            send_sem=link_send.at[link, step % AHEAD],
            recv_sem=link_recv.at[link, step % SLOTS],
            device_id=(device(sy, sz, core), column),
            device_id_type=MESH,
        )

    def last_copy(link):
        place = place_of(SENT[link][STEPS - 1], core)
        sy, sz = SHIFT[link]
        return pltpu.make_async_remote_copy(
            src_ref=gathered.at[place],
            dst_ref=gathered.at[place],
            send_sem=last_sem.at[0],
            recv_sem=last_sem.at[1],
            device_id=(device(sy, sz, 1 - core), column),
            device_id_type=MESH,
        )

    def core_copy(place):
        return pltpu.make_async_remote_copy(
            src_ref=gathered.at[place],
            dst_ref=gathered.at[place],
            send_sem=core_send,
            recv_sem=core_recv,
            device_id=(device(0, 0, 1 - core), column),
            device_id_type=MESH,
        )

    def normalise(tiles):
        def body(i, _):
            at = pl.multiple_of(i * 16, 16)
            to = pl.multiple_of(me * BLOCK + i * 16, 16)
            for j in tiles:
                lanes = slice(j * 128, (j + 1) * 128)
                gathered[pl.ds(to, 16), lanes] = (first[pl.ds(at, 16), lanes] * inverse[j]).astype(jnp.bfloat16)
            return 0

        lax.fori_loop(0, BLOCK // 16, body, 0)

    def normalise_early():
        for link, (sy, sz) in enumerate(SHIFT):
            for i in range(EARLY // 16):
                to = pl.multiple_of(device(-sy, -sz, core) * BLOCK + i * 16, 16)
                for j in range(9):
                    lanes = slice(j * 128, (j + 1) * 128)
                    values = early_rows[link, i * 16 : (i + 1) * 16, lanes] * inverse[j]
                    gathered[pl.ds(to, 16), lanes] = values.astype(jnp.bfloat16)

    arrived = set()

    def receive(link, step):
        if (link, step) in arrived:
            return
        arrived.add((link, step))
        item = arriving(link, step)
        link_copy(link, step, item).wait_recv()
        if step < STEPS - 1:
            core_copy(place_of(item, core)).start()

    all_sums(sums_early, 0).wait_recv()
    grand(sums_early, early)
    normalise(early)

    for step in range(STEPS):
        for link in range(3):
            if step >= AHEAD:
                link_copy(link, step - AHEAD, SENT[link][step - AHEAD]).wait_send()
            item = SENT[link][step]
            if item[:2] != (0, 0):
                for arrival in needed(item):
                    receive(*arrival)
            link_copy(link, step, item).start()
            if step == STEPS - 1:
                last_copy(link).start()
        if step == 0:

            @pl.when(jnp.logical_not(at_gate))
            def _():
                send_row().start()

            all_sums(sums_late, 1).wait_recv()
            grand(sums_late, late)
            normalise(late)
        if step == 1:
            all_early().wait_recv()
            normalise_early()
        if step == 3:
            for sy, sz in SHIFT:
                core_copy(place_of((-sy, -sz, (0, EARLY), ALL), core)).start()
        if step in (1, 2):
            core_copy(place_of((0, 0, ((step - 1) * HALF, step * HALF), ALL), core)).start()
        if step == GAIN_STEPS[0]:

            @pl.when(at_gate)
            def _():
                all_rows().wait_recv()
                pl.semaphore_wait(barrier, 7)
                for k in range(1, 8):
                    send_group(k).start()

        if step == GAIN_STEPS[1]:

            @pl.when(at_gate)
            def _():
                all_groups().wait_recv()
                compose()

        if step == GAIN_STEPS[2]:

            @pl.when(at_gate)
            def _():
                for to in spread:
                    send_gain(to).start()

        if step == GAIN_STEPS[3]:

            @pl.when(jnp.logical_and(jnp.logical_not(at_gate), core == GATE % 2))
            def _():
                send_gain(me).wait_recv()
                send_gain(device(0, 0, 1 - core)).start()

        if step >= AHEAD:
            for link in range(3):
                receive(link, step - AHEAD)

    for step in range(STEPS - AHEAD, STEPS):
        for link in range(3):
            receive(link, step)
    for step in range(STEPS - AHEAD, STEPS):
        for link in range(3):
            link_copy(link, step, SENT[link][step]).wait_send()
    all_early().wait_send()
    all_sums(sums_early, 0).wait_send()
    all_sums(sums_late, 1).wait_send()

    @pl.when(core != GATE % 2)
    def _():
        send_gain(me).wait_recv()

    @pl.when(at_gate)
    def _():
        all_groups().wait_send()
        gains_sent = gathered.at[pl.ds(0, 448), pl.ds(0, 128)]
        pltpu.make_async_copy(gains_sent, gains_sent, gain_sem.at[0]).wait()

    @pl.when(jnp.logical_not(at_gate))
    def _():
        send_row().wait_send()

        @pl.when(core == GATE % 2)
        def _():
            send_gain(me).wait_send()

    half = core_copy((pl.ds(0, 8 * BLOCK - 3 * LAST), pl.ds(0, 1152)))
    half.wait_send()
    half.wait_recv()
    rows = gathered.at[pl.ds(0, 3 * LAST), :]
    for n in range(2):
        pltpu.make_async_copy(rows, rows, last_sem.at[n]).wait()


def write_kernel(gathered, *rest):
    small, (query, key, value), outs, sem = rest[:4], rest[4:7], rest[7:11], rest[11]
    parts = 4
    rows = gathered.shape[0] // parts
    for part in range(parts):
        at = pl.ds(part * rows, rows)
        pltpu.make_async_copy(gathered.at[at, pl.ds(0, 896)], query.at[at, :], sem.at[0]).start()
    others = [
        pltpu.make_async_copy(gathered.at[:, pl.ds(896, 128)], key, sem.at[1]),
        pltpu.make_async_copy(gathered.at[:, pl.ds(1024, 128)], value, sem.at[2]),
    ]
    for source, target in zip(small, outs):
        others.append(pltpu.make_async_copy(source, target, sem.at[len(others) + 1]))
    for copy in others:
        copy.start()
    pltpu.make_async_copy(gathered.at[:, pl.ds(0, 896)], query, sem.at[0]).wait()
    for copy in others:
        copy.wait()


def shards(
    one_query,
    other_query,
    one_key,
    other_key,
    one_value,
    other_value,
    mix_share,
    norm_train,
    norm_step,
):
    dma = pltpu.SemaphoreType.DMA
    f32, bf16 = jnp.float32, jnp.bfloat16
    inputs = [
        pltpu.with_memory_space_constraint(x, HBM)
        for x in (
            one_query,
            other_query,
            one_key,
            other_key,
            one_value,
            other_value,
            mix_share.reshape(1, 448),
            norm_train.reshape(1, 56),
            norm_step.reshape(1, 56),
        )
    ]
    small = (
        jax.ShapeDtypeStruct((7, 128), f32),
        jax.ShapeDtypeStruct((1, 128), f32),
        jax.ShapeDtypeStruct((1, 128), f32),
        jax.ShapeDtypeStruct((56, 128), bf16),
    )
    gathered, *rest = pl.pallas_call(
        gather_kernel,
        out_shape=(jax.ShapeDtypeStruct((7168, 1152), bf16), *small),
        in_specs=[pl.BlockSpec(memory_space=HBM)] * 9,
        out_specs=(pl.BlockSpec(memory_space=VMEM),) * 5,
        scratch_shapes=[
            pltpu.VMEM((448, 1152), f32),
            pltpu.VMEM((448, 1152), f32),
            pltpu.VMEM((1, 448), f32),
            pltpu.VMEM((2, 1, 56), f32),
            pltpu.VMEM((1, 512), f32),
            pltpu.VMEM((512, 128), f32),
            pltpu.VMEM((16, 7, 1, 128), f32),
            pltpu.VMEM((16, 2, 1, 128), f32),
            pltpu.VMEM((9, 1, 128), f32),
            pltpu.VMEM((8, 128), f32),
            pltpu.VMEM((8, 16, 1, 128), f32),
            pltpu.VMEM((56, 128), f32),
            pltpu.VMEM((3, EARLY, 1152), f32),
            dma((BLOCK // PIECE + 1,)),
            dma((2,)),
            pltpu.SemaphoreType.REGULAR,
            dma((2,)),
            dma((2,)),
            dma((2,)),
            dma((2,)),
            dma((2,)),
            dma((3, AHEAD)),
            dma((3, SLOTS)),
            dma,
            dma,
            dma((2,)),
            dma((2,)),
        ],
        compiler_params=pltpu.CompilerParams(
            collective_id=0, has_side_effects=True, vmem_limit_bytes=32 << 20
        ),
    )(*inputs)
    query, key, value, *outs = pl.pallas_call(
        write_kernel,
        out_shape=(
            jax.ShapeDtypeStruct((7168, 896), bf16),
            jax.ShapeDtypeStruct((7168, 128), bf16),
            jax.ShapeDtypeStruct((7168, 128), bf16),
            *small,
        ),
        in_specs=[pl.BlockSpec(memory_space=VMEM)] * 5,
        out_specs=(pl.BlockSpec(memory_space=HBM),) * 7,
        scratch_shapes=[dma((7,))],
        compiler_params=pltpu.CompilerParams(vmem_limit_bytes=20 << 20),
    )(gathered, *rest)
    return (query, key, value, *(x.reshape(-1) for x in outs))


def solution(mesh):
    in_specs = (
        P("rows", "width"),
        P("rows", "width"),
        P("rows", "width"),
        P("rows", "width"),
        P("rows", "width"),
        P("rows", "width"),
        P("rows"),
        P(("rows", "width")),
        P(("rows", "width")),
    )
    out_specs = (
        P(None, "width"),
        P(None, "width"),
        P(None, "width"),
        P("width"),
        P("width"),
        P("width"),
        P(),
    )
    return jax.shard_map(shards, mesh=mesh, in_specs=in_specs, out_specs=out_specs, check_vma=False)
```

```python
import functools

import jax
import jax.numpy as jnp
from jax import lax
from jax.experimental import pallas as pl
from jax.experimental.pallas import tpu as pltpu
from jax.sharding import PartitionSpec as P

MESH = pl.DeviceIdType.MESH
HBM = pltpu.MemorySpace.HBM
VMEM = pltpu.MemorySpace.VMEM

BLOCK = 448
HALF = 224
PIECE = 112
QUERY = (0, 896)
KEYVALUE = (896, 256)
ALL = (0, 1152)
EARLY = 32
LAST = 8
LOW = ((EARLY, 96), (96, 160), (160, 224))
HIGH = ((224, 304), (304, 368), (368, 448))


def own(*parts):
    return [(0, 0, rows, columns) for rows, columns in parts]


def relay(dy, dz, *rows):
    return [(dy, dz, r, ALL) for r in rows]


UP = (
    own(((EARLY, 160), KEYVALUE), (LOW[0], QUERY), (LOW[1], QUERY), (LOW[2], ALL), *((r, ALL) for r in HIGH))
    + relay(-1, 0, (0, 96), *LOW[1:])
    + relay(0, 1, (224, 304), (304, 376))
    + relay(-1, 1, (0, 96), (96, 160), (160, 200), (200, 216), (216, 224))
)
DOWN = (
    own(((224, 368), KEYVALUE), (HIGH[0], QUERY), (HIGH[1], QUERY), (HIGH[2], ALL), *((r, ALL) for r in LOW))
    + relay(1, 0, *HIGH)
    + relay(0, 1, (0, 80), (80, 152))
    + relay(1, 1, (224, 304), (304, 368), (368, 424), (424, 440), (440, 448))
)
ACROSS = (
    own(
        ((EARLY, 160), KEYVALUE),
        (LOW[0], QUERY),
        (HIGH[0], ALL),
        (LOW[1], QUERY),
        (HIGH[1], ALL),
        (LOW[2], ALL),
        (HIGH[2], ALL),
    )
    + relay(-1, 0, (0, 96))
    + relay(1, 0, HIGH[0])
    + relay(-1, 0, LOW[1])
    + relay(1, 0, HIGH[1])
    + relay(-1, 0, LOW[2])
    + relay(1, 0, HIGH[2])
    + relay(-1, 0, (376, 448))
    + relay(1, 0, (152, 200), (200, 216), (216, 224))
)
SENT = (UP, DOWN, ACROSS)
SHIFT = ((1, 0), (-1, 0), (0, 1))
STEPS = len(UP)
AHEAD = 2
SLOTS = 2 * AHEAD + 2
GATE = 1
GAIN_STEPS = (5, 8, 9, 12)
FARTHEST = ((2, 1), (2, 0), (1, 1), (3, 1), (1, 0), (3, 0), (0, 1), (0, 0))


def arriving(link, step):
    dy, dz, rows, columns = SENT[link][step]
    sy, sz = SHIFT[link]
    return ((dy - sy) % 4, (dz - sz) % 2, rows, columns)


ARRIVALS = [(l, s) for s in range(STEPS) for l in range(3)]


def needed(item):
    dy, dz, rows, _ = item
    for l, s in ARRIVALS:
        ay, az, have, _ = arriving(l, s)
        if (ay, az) == (dy % 4, dz % 2) and have[0] < rows[1] and rows[0] < have[1]:
            yield l, s


def gather_kernel(
    one_query,
    other_query,
    one_key,
    other_key,
    one_value,
    other_value,
    share_input,
    train_input,
    step_input,
    gathered,
    scale_query,
    scale_key,
    scale_value,
    gain,
    first,
    second,
    share,
    gains,
    share_row,
    share_tile,
    sums_late,
    sums_early,
    inverse,
    gain_tile,
    gain_rows,
    gain_flat,
    early_rows,
    load_sem,
    small_sem,
    entered,
    sum_send,
    sum_recv,
    row_sem,
    gate_sem,
    gain_sem,
    link_send,
    link_recv,
    core_send,
    core_recv,
    early_sem,
    last_sem,
):
    me = lax.axis_index("rows")
    column = lax.axis_index("width")
    core = lax.rem(me, 2)
    y = lax.rem(me // 2, 4)
    z = me // 8

    def device(dy, dz, on):
        return lax.rem(z + dz + 2, 2) * 8 + lax.rem(y + dy + 4, 4) * 2 + on

    at_gate = me == GATE
    barrier = pltpu.get_barrier_semaphore()
    others = [(dy, dz, on) for dy, dz in FARTHEST for on in (0, 1) if (dy, dz, on) != (0, 0, 0)]
    def signal(peers):
        for dy, dz, on in peers:
            peer = device(dy, dz, lax.rem(core + on, 2))

            @pl.when(peer != GATE)
            def _():
                pl.semaphore_signal(barrier, inc=1, device_id=(peer, column), device_id_type=MESH)

    signal(others[:6])

    small = [
        pltpu.make_async_copy(share_input, share, small_sem.at[0]),
        pltpu.make_async_copy(train_input, gains.at[0], small_sem.at[1]),
        pltpu.make_async_copy(step_input, gains.at[1], small_sem.at[1]),
    ]
    pieces = BLOCK // PIECE
    small[0].start()
    for source, target, at in (
        (one_key, first, 896),
        (other_key, second, 896),
        (one_value, first, 1024),
        (other_value, second, 1024),
    ):
        pltpu.make_async_copy(source, target.at[:, pl.ds(at, 128)], load_sem.at[pieces]).start()
    for piece in range(pieces):
        rows = pl.ds(piece * PIECE, PIECE)
        for source, target in ((one_query, first), (other_query, second)):
            pltpu.make_async_copy(source.at[rows, :], target.at[rows, pl.ds(0, 896)], load_sem.at[piece]).start()
    for copy in small[1:]:
        copy.start()

    signal(others[6:])

    @pl.when(at_gate)
    def _():
        for k in range(1, 8):
            pl.semaphore_signal(barrier, inc=1, device_id=(me, lax.rem(column + k, 8)), device_id_type=MESH)

    def loaded(number, rows, columns):
        place = (pl.ds(0, rows), pl.ds(0, columns))
        pltpu.make_async_copy(first.at[place], second.at[place], load_sem.at[number]).wait()

    small[0].wait()
    share_row[...] = jnp.zeros_like(share_row)
    share_row[:, 0:BLOCK] = share[...]
    for part in range(4):
        lanes = share_row[:, part * 128 : (part + 1) * 128]
        share_tile[pl.ds(part * 128, 128), :] = jnp.transpose(jnp.broadcast_to(lanes, (128, 128)))

    def mix(start, rows, tiles, total):
        def body(i, total):
            total = list(total)
            for part in range(2):
                at = pl.ds(pl.multiple_of(start + i * 16 + part * 8, 8), 8)
                mine = share_tile[at, :]
                rest = 1.0 - mine
                for n, j in enumerate(tiles):
                    lanes = slice(j * 128, (j + 1) * 128)
                    result = mine * first[at, lanes] + rest * second[at, lanes]
                    first[at, lanes] = result
                    total[n] = total[n] + result * result
            return tuple(total)

        return lax.fori_loop(0, rows // 16, body, total, unroll=2 if len(tiles) == 2 else 1)

    def zeros(n):
        return tuple(jnp.zeros((8, 128), jnp.float32) for _ in range(n))

    def send_sum(sums, n, dy, dz, on):
        return pltpu.make_async_remote_copy(
            src_ref=sums.at[me],
            dst_ref=sums.at[me],
            send_sem=sum_send.at[n],
            recv_sem=sum_recv.at[n],
            device_id=(device(dy, dz, lax.rem(core + on, 2)), column),
            device_id_type=MESH,
        )

    def all_sums(sums, n):
        return pltpu.make_async_remote_copy(
            src_ref=sums.at[pl.ds(0, 15)],
            dst_ref=sums.at[pl.ds(0, 15)],
            send_sem=sum_send.at[n],
            recv_sem=sum_recv.at[n],
            device_id=(device(0, 0, 1 - core), column),
            device_id_type=MESH,
        )

    def grand(sums, tiles):
        total = [sums[0, n] for n in range(len(tiles))]
        for other in range(1, 16):
            total = [t + sums[other, n] for n, t in enumerate(total)]
        for j, t in zip(tiles, total):
            scale = jnp.sqrt(t)
            if j < 7:
                scale_query[j : j + 1, :] = scale
            elif j == 7:
                scale_key[...] = scale
            else:
                scale_value[...] = scale
            inverse[j] = 1.0 / scale

    late, early = tuple(range(7)), (7, 8)

    loaded(pieces, BLOCK, 512)
    for n, t in enumerate(mix(0, BLOCK, early, zeros(2))):
        sums_early[me, n] = jnp.sum(t, axis=0, keepdims=True)

    @pl.when(jnp.logical_not(at_gate))
    def _():
        pl.semaphore_wait(barrier, 15)

    @pl.when(me == GATE - 1)
    def _():
        pl.semaphore_signal(entered, inc=1, device_id=(GATE, column), device_id_type=MESH)

    @pl.when(at_gate)
    def _():
        pl.semaphore_wait(entered, 1)

    for to in others:
        send_sum(sums_early, 0, *to).start()
    total = zeros(7)
    for piece in range(pieces):
        loaded(piece, 2 * PIECE, 896)
        total = mix(piece * PIECE, PIECE, late, total)
    for n, t in enumerate(total):
        sums_late[me, n] = jnp.sum(t, axis=0, keepdims=True)
    for to in others:
        send_sum(sums_late, 1, *to).start()

    def early_copy(link):
        sy, sz = SHIFT[link]
        return pltpu.make_async_remote_copy(
            src_ref=first.at[pl.ds(0, EARLY), :],
            dst_ref=early_rows.at[link],
            send_sem=early_sem.at[0],
            recv_sem=early_sem.at[1],
            device_id=(device(sy, sz, core), column),
            device_id_type=MESH,
        )

    def all_early():
        return pltpu.make_async_remote_copy(
            src_ref=early_rows,
            dst_ref=early_rows,
            send_sem=early_sem.at[0],
            recv_sem=early_sem.at[1],
            device_id=(device(0, 0, 1 - core), column),
            device_id_type=MESH,
        )

    for link in range(3):
        early_copy(link).start()

    pltpu.make_async_copy(gains, gains, small_sem.at[1]).wait()
    gain_tile[...] = jnp.zeros_like(gain_tile)
    gain_tile[0:1, 0:56] = (gains[0] + gains[1]).astype(jnp.bfloat16).astype(jnp.float32)
    place = lax.rem(56 * (lax.rem(me, 2) * 8 + column), 128)
    gain_rows[column, me] = pltpu.roll(gain_tile[...], place, 1)[0:1, :]

    def send_row():
        return pltpu.make_async_remote_copy(
            src_ref=gain_rows.at[column, me],
            dst_ref=gain_rows.at[column, me],
            send_sem=row_sem.at[0],
            recv_sem=row_sem.at[1],
            device_id=(GATE, column),
            device_id_type=MESH,
        )

    def all_rows():
        return pltpu.make_async_remote_copy(
            src_ref=gain_rows.at[column, pl.ds(0, 15)],
            dst_ref=gain_rows.at[column, pl.ds(0, 15)],
            send_sem=row_sem.at[0],
            recv_sem=row_sem.at[1],
            device_id=(GATE - 1, column),
            device_id_type=MESH,
        )

    def send_group(k):
        return pltpu.make_async_remote_copy(
            src_ref=gain_rows.at[column],
            dst_ref=gain_rows.at[column],
            send_sem=gate_sem.at[0],
            recv_sem=gate_sem.at[1],
            device_id=(GATE, lax.rem(column + k, 8)),
            device_id_type=MESH,
        )

    def all_groups():
        return pltpu.make_async_remote_copy(
            src_ref=gain_rows.at[pl.ds(0, 7)],
            dst_ref=gain_rows.at[pl.ds(0, 7)],
            send_sem=gate_sem.at[0],
            recv_sem=gate_sem.at[1],
            device_id=(GATE - 1, column),
            device_id_type=MESH,
        )

    def send_gain(to):
        return pltpu.make_async_remote_copy(
            src_ref=gain,
            dst_ref=gain,
            send_sem=gain_sem.at[0],
            recv_sem=gain_sem.at[1],
            device_id=(to, column),
            device_id_type=MESH,
        )

    def compose():
        lane = lax.broadcasted_iota(jnp.int32, (1, 128), 1)
        for group in range(8):
            rows = [jnp.zeros((1, 128), jnp.float32) for _ in range(8)]
            for j in range(16):
                values = gain_rows[j % 8, group * 2 + j // 8]
                row, at = (56 * j) // 128, (56 * j) % 128
                rows[row] = jnp.where((lane >= at) & (lane < at + 56), values, rows[row])
                if at + 56 > 128:
                    rows[row + 1] = jnp.where(lane < at + 56 - 128, values, rows[row + 1])
            for row in range(7):
                gain_flat[group * 7 + row : group * 7 + row + 1, :] = rows[row]
        gain[...] = gain_flat[...].astype(jnp.bfloat16)

    spread = [to for to in range(16) if to % 2 == GATE % 2 and to != GATE] + [GATE - 1]

    def place_of(item, on):
        dy, dz, (low, high), (left, width) = item
        start = pl.multiple_of(device(dy, dz, on) * BLOCK + low, 8)
        return (pl.ds(start, high - low), pl.ds(left, width))

    def link_copy(link, step, item):
        place = place_of(item, core)
        sy, sz = SHIFT[link]
        return pltpu.make_async_remote_copy(
            src_ref=gathered.at[place],
            dst_ref=gathered.at[place],
            send_sem=link_send.at[link, step % AHEAD],
            recv_sem=link_recv.at[link, step % SLOTS],
            device_id=(device(sy, sz, core), column),
            device_id_type=MESH,
        )

    def last_copy(link):
        place = place_of(SENT[link][STEPS - 1], core)
        sy, sz = SHIFT[link]
        return pltpu.make_async_remote_copy(
            src_ref=gathered.at[place],
            dst_ref=gathered.at[place],
            send_sem=last_sem.at[0],
            recv_sem=last_sem.at[1],
            device_id=(device(sy, sz, 1 - core), column),
            device_id_type=MESH,
        )

    def core_copy(place):
        return pltpu.make_async_remote_copy(
            src_ref=gathered.at[place],
            dst_ref=gathered.at[place],
            send_sem=core_send,
            recv_sem=core_recv,
            device_id=(device(0, 0, 1 - core), column),
            device_id_type=MESH,
        )

    def normalise(tiles):
        def body(i, _):
            at = pl.multiple_of(i * 16, 16)
            to = pl.multiple_of(me * BLOCK + i * 16, 16)
            for j in tiles:
                lanes = slice(j * 128, (j + 1) * 128)
                gathered[pl.ds(to, 16), lanes] = (first[pl.ds(at, 16), lanes] * inverse[j]).astype(jnp.bfloat16)
            return 0

        lax.fori_loop(0, BLOCK // 16, body, 0)

    def normalise_early():
        for link, (sy, sz) in enumerate(SHIFT):
            for i in range(EARLY // 16):
                to = pl.multiple_of(device(-sy, -sz, core) * BLOCK + i * 16, 16)
                for j in range(9):
                    lanes = slice(j * 128, (j + 1) * 128)
                    values = early_rows[link, i * 16 : (i + 1) * 16, lanes] * inverse[j]
                    gathered[pl.ds(to, 16), lanes] = values.astype(jnp.bfloat16)

    arrived = set()

    def receive(link, step):
        if (link, step) in arrived:
            return
        arrived.add((link, step))
        item = arriving(link, step)
        link_copy(link, step, item).wait_recv()
        if step < STEPS - 1:
            core_copy(place_of(item, core)).start()

    all_sums(sums_early, 0).wait_recv()
    grand(sums_early, early)
    normalise(early)

    for step in range(STEPS):
        for link in range(3):
            if step >= AHEAD:
                link_copy(link, step - AHEAD, SENT[link][step - AHEAD]).wait_send()
            item = SENT[link][step]
            if item[:2] != (0, 0):
                for arrival in needed(item):
                    receive(*arrival)
            link_copy(link, step, item).start()
            if step == STEPS - 1:
                last_copy(link).start()
        if step == 0:

            @pl.when(jnp.logical_not(at_gate))
            def _():
                send_row().start()

            all_sums(sums_late, 1).wait_recv()
            grand(sums_late, late)
            normalise(late)
        if step == 1:
            all_early().wait_recv()
            normalise_early()
        if step == 3:
            for sy, sz in SHIFT:
                core_copy(place_of((-sy, -sz, (0, EARLY), ALL), core)).start()
        if step in (1, 2):
            core_copy(place_of((0, 0, ((step - 1) * HALF, step * HALF), ALL), core)).start()
        if step == GAIN_STEPS[0]:

            @pl.when(at_gate)
            def _():
                all_rows().wait_recv()
                pl.semaphore_wait(barrier, 7)
                for k in range(1, 8):
                    send_group(k).start()

        if step == GAIN_STEPS[1]:

            @pl.when(at_gate)
            def _():
                all_groups().wait_recv()
                compose()

        if step == GAIN_STEPS[2]:

            @pl.when(at_gate)
            def _():
                for to in spread:
                    send_gain(to).start()

        if step == GAIN_STEPS[3]:

            @pl.when(jnp.logical_and(jnp.logical_not(at_gate), core == GATE % 2))
            def _():
                send_gain(me).wait_recv()
                send_gain(device(0, 0, 1 - core)).start()

        if step >= AHEAD:
            for link in range(3):
                receive(link, step - AHEAD)

    for step in range(STEPS - AHEAD, STEPS):
        for link in range(3):
            receive(link, step)
    for step in range(STEPS - AHEAD, STEPS):
        for link in range(3):
            link_copy(link, step, SENT[link][step]).wait_send()
    all_early().wait_send()
    all_sums(sums_early, 0).wait_send()
    all_sums(sums_late, 1).wait_send()

    @pl.when(core != GATE % 2)
    def _():
        send_gain(me).wait_recv()

    @pl.when(at_gate)
    def _():
        all_groups().wait_send()
        gains_sent = gathered.at[pl.ds(0, 448), pl.ds(0, 128)]
        pltpu.make_async_copy(gains_sent, gains_sent, gain_sem.at[0]).wait()

    @pl.when(jnp.logical_not(at_gate))
    def _():
        send_row().wait_send()

        @pl.when(core == GATE % 2)
        def _():
            send_gain(me).wait_send()

    half = core_copy((pl.ds(0, 8 * BLOCK - 3 * LAST), pl.ds(0, 1152)))
    half.wait_send()
    half.wait_recv()
    rows = gathered.at[pl.ds(0, 3 * LAST), :]
    for n in range(2):
        pltpu.make_async_copy(rows, rows, last_sem.at[n]).wait()


def write_kernel(gathered, *rest):
    small, (query, key, value), outs, sem = rest[:4], rest[4:7], rest[7:11], rest[11]
    parts = 4
    rows = gathered.shape[0] // parts
    for part in range(parts):
        at = pl.ds(part * rows, rows)
        pltpu.make_async_copy(gathered.at[at, pl.ds(0, 896)], query.at[at, :], sem.at[0]).start()
    others = [
        pltpu.make_async_copy(gathered.at[:, pl.ds(896, 128)], key, sem.at[1]),
        pltpu.make_async_copy(gathered.at[:, pl.ds(1024, 128)], value, sem.at[2]),
    ]
    for source, target in zip(small, outs):
        others.append(pltpu.make_async_copy(source, target, sem.at[len(others) + 1]))
    for copy in others:
        copy.start()
    pltpu.make_async_copy(gathered.at[:, pl.ds(0, 896)], query, sem.at[0]).wait()
    for copy in others:
        copy.wait()


def shards(
    one_query,
    other_query,
    one_key,
    other_key,
    one_value,
    other_value,
    mix_share,
    norm_train,
    norm_step,
):
    dma = pltpu.SemaphoreType.DMA
    f32, bf16 = jnp.float32, jnp.bfloat16
    inputs = [
        pltpu.with_memory_space_constraint(x, HBM)
        for x in (
            one_query,
            other_query,
            one_key,
            other_key,
            one_value,
            other_value,
            mix_share.reshape(1, 448),
            norm_train.reshape(1, 56),
            norm_step.reshape(1, 56),
        )
    ]
    small = (
        jax.ShapeDtypeStruct((7, 128), f32),
        jax.ShapeDtypeStruct((1, 128), f32),
        jax.ShapeDtypeStruct((1, 128), f32),
        jax.ShapeDtypeStruct((56, 128), bf16),
    )
    gathered, *rest = pl.pallas_call(
        gather_kernel,
        out_shape=(jax.ShapeDtypeStruct((7168, 1152), bf16), *small),
        in_specs=[pl.BlockSpec(memory_space=HBM)] * 9,
        out_specs=(pl.BlockSpec(memory_space=VMEM),) * 5,
        scratch_shapes=[
            pltpu.VMEM((448, 1152), f32),
            pltpu.VMEM((448, 1152), f32),
            pltpu.VMEM((1, 448), f32),
            pltpu.VMEM((2, 1, 56), f32),
            pltpu.VMEM((1, 512), f32),
            pltpu.VMEM((512, 128), f32),
            pltpu.VMEM((16, 7, 1, 128), f32),
            pltpu.VMEM((16, 2, 1, 128), f32),
            pltpu.VMEM((9, 1, 128), f32),
            pltpu.VMEM((8, 128), f32),
            pltpu.VMEM((8, 16, 1, 128), f32),
            pltpu.VMEM((56, 128), f32),
            pltpu.VMEM((3, EARLY, 1152), f32),
            dma((BLOCK // PIECE + 1,)),
            dma((2,)),
            pltpu.SemaphoreType.REGULAR,
            dma((2,)),
            dma((2,)),
            dma((2,)),
            dma((2,)),
            dma((2,)),
            dma((3, AHEAD)),
            dma((3, SLOTS)),
            dma,
            dma,
            dma((2,)),
            dma((2,)),
        ],
        compiler_params=pltpu.CompilerParams(
            collective_id=0, has_side_effects=True, vmem_limit_bytes=32 << 20
        ),
    )(*inputs)
    query, key, value, *outs = pl.pallas_call(
        write_kernel,
        out_shape=(
            jax.ShapeDtypeStruct((7168, 896), bf16),
            jax.ShapeDtypeStruct((7168, 128), bf16),
            jax.ShapeDtypeStruct((7168, 128), bf16),
            *small,
        ),
        in_specs=[pl.BlockSpec(memory_space=VMEM)] * 5,
        out_specs=(pl.BlockSpec(memory_space=HBM),) * 7,
        scratch_shapes=[dma((7,))],
        compiler_params=pltpu.CompilerParams(vmem_limit_bytes=20 << 20),
    )(gathered, *rest)
    return (query, key, value, *(x.reshape(-1) for x in outs))


def solution(mesh):
    in_specs = (
        P("rows", "width"),
        P("rows", "width"),
        P("rows", "width"),
        P("rows", "width"),
        P("rows", "width"),
        P("rows", "width"),
        P("rows"),
        P(("rows", "width")),
        P(("rows", "width")),
    )
    out_specs = (
        P(None, "width"),
        P(None, "width"),
        P(None, "width"),
        P("width"),
        P("width"),
        P("width"),
        P(),
    )
    return jax.shard_map(shards, mesh=mesh, in_specs=in_specs, out_specs=out_specs, check_vma=False)
```
